128 devices in a mesh: aa: 16 (over z_hi, x, core), ba: 8 (over z_lo, y).
Axes of the slice: x: 4, y: 4, z: 4 (z_hi: 2, z_lo: 2; z = z_hi * 2 + z_lo), core: 2. Of those that a mesh axis runs over, the one named last changes fastest.
Arguments:
- cotangent: bfloat16 [1, 20, 64, 64, 2048], P(None, None, 'aa', 'ba'), may hold values from -6 to 6
- pre_activations: bfloat16 [2, 1, 20, 64, 64, 2048], P(None, None, None, 'aa', 'ba'), may hold values from -6 to 6
- spectral_weights: bfloat16 [2, 2, 20, 20, 24, 6912], P(None, None, None, None, 'ba', 'aa'), may hold values from -6 to 6
- skip_weights: bfloat16 [2, 20, 20], replicated, may hold values from -1.25 to 1.25
- lift_weights: float32 [20], replicated, may hold values from -1.25 to 1.25
Outputs:
- perm_grad: float32 [1, 64, 64, 2048], P(None, 'aa', 'ba')
The draws below stay inside these ranges and needn't reach their ends.
All inputs are finite; a program needn't handle non-finite values.
Results may differ from the reference program's by a relative error of at most 0.023.
Values may be sent and summed in bfloat16 or wider, within the bound.
A program may use at most 192 MiB of HBM per device.

```python
import math
import jax
import jax.numpy as jnp
from jax import lax

C = 20
NX = 64
NY = 64
NZ = 64
NT = 32
KX = 24
KY = 24
KZ = 24
KT = 12
LAYERS = 2
B = 1


def level_of(key, extent, cuts, smallest, top_value):
    factor_of = 1.0
    for dim, blocks in cuts:
        steps = jax.random.uniform(jax.random.fold_in(jax.random.fold_in(key, 6), dim), (blocks,), jnp.float32, smallest / len(cuts), top_value / len(cuts))
        factor_of = factor_of * jnp.repeat(jnp.exp(steps), extent[dim] // blocks).reshape((-1,) + (1,) * (len(extent) - 1 - dim))
    return factor_of


def normal_values(key, dims, deviation, reach, pieces=(), kind=jnp.bfloat16):
    entries = deviation * jax.random.normal(key, dims, jnp.float32)
    if pieces:
        entries = entries * level_of(key, dims, pieces, -0.22, 0.18)
    return jnp.clip(entries, -reach, reach).astype(kind)


def setup_inputs(seed: int = 0) -> dict:
    key_of = jax.random.split(jax.random.key(seed), 6)
    return {
        "cotangent": normal_values(key_of[0], (B, C, NX, NY, NZ * NT), 1.0, 6.0, ((2, 16), (3, 8))),
        "pre_activations": normal_values(key_of[1], (LAYERS, B, C, NX, NY, NZ * NT), 1.0, 6.0, ((3, 16), (4, 8))),
        "spectral_weights": normal_values(key_of[2], (LAYERS, 2, C, C, KX, KZ * KT * KY), ((NX * NY * NZ * NT) ** 0.5 * (KX * KY * KZ * KT * C) ** -0.5), 6.0, ((4, 8), (5, 16))),
        "skip_weights": normal_values(key_of[3], (LAYERS, C, C), C ** -0.5, 1.25),
        "lift_weights": normal_values(key_of[4], (C,), C ** -0.5, 1.25, (), jnp.float32),
    }


def gelu_slope(values):
    normal_cdf = 0.5 * (1.0 + lax.erf(values / math.sqrt(2.0)))
    density = jnp.exp(-0.5 * values * values) / math.sqrt(2.0 * math.pi)
    return normal_cdf + values * density

def round_complex(values):
    real_part = lax.optimization_barrier(values.real.astype(jnp.bfloat16)).astype(jnp.float32)
    imag_part = lax.optimization_barrier(values.imag.astype(jnp.bfloat16)).astype(jnp.float32)
    return lax.complex(real_part, imag_part)

def kept_index(total_count, length):
    return jnp.concatenate([jnp.arange(total_count // 2, dtype=jnp.int32), jnp.arange(length - total_count // 2, length, dtype=jnp.int32)])

def forward_field(field):
    values = field.astype(jnp.float32).reshape(NX, NY, NZ, NT)
    spectrum = jnp.fft.fft2(values, axes=(2, 3))
    spectrum = jnp.take(spectrum, kept_index(KZ, NZ), axis=2)
    spectrum = round_complex(spectrum[:, :, :, :KT])
    spectrum = round_complex(jnp.take(jnp.fft.fft(spectrum, axis=0), kept_index(KX, NX), axis=0))
    spectrum = round_complex(jnp.take(jnp.fft.fft(spectrum, axis=1), kept_index(KY, NY), axis=1))
    return spectrum

def inverse_field(mode_values, rounded):
    gridded = jnp.zeros((KX, NY, KZ, KT), mode_values.dtype).at[:, kept_index(KY, NY)].set(mode_values)
    gridded = jnp.fft.ifft(gridded, axis=1)
    if rounded:
        gridded = round_complex(gridded)
    spread = jnp.zeros((NX, NY, KZ, KT), mode_values.dtype).at[kept_index(KX, NX)].set(gridded)
    spread = jnp.fft.ifft(spread, axis=0)
    if rounded:
        spread = round_complex(spread)
    plane = jnp.zeros((NX, NY, NZ, NT), mode_values.dtype).at[:, :, kept_index(KZ, NZ), :KT].set(spread)
    return jnp.fft.ifft2(plane, axes=(2, 3)).real.reshape(NX, NY, NZ * NT)

def mix_modes(spectrum, weights):
    shaped = weights.astype(jnp.float32).reshape(2, C, C, KX, KZ, KT, KY)
    conj_weights = lax.complex(shaped[0], -shaped[1])
    return jnp.einsum('oxyzt,oixzty->ixyzt', spectrum, conj_weights)

def sample_grad(cot_sample, pre_sample, spectral_weights, skip_weights, lift_weights):
    incoming = cot_sample.astype(jnp.float32)
    for level_index in range(LAYERS - 1, -1, -1):
        grad_pre = (incoming * gelu_slope(pre_sample[level_index].astype(jnp.float32))).astype(jnp.bfloat16)
        spectrum = lax.map(forward_field, grad_pre)
        mode_values = mix_modes(spectrum, spectral_weights[level_index])
        if level_index > 0:
            mode_values = round_complex(mode_values)
            spectral = lax.map(lambda entry: inverse_field(entry, True), mode_values)
        else:
            spectral = lax.map(lambda entry: inverse_field(entry, False), mode_values)
        skip_term = jnp.einsum('oxyz,oi->ixyz', grad_pre.astype(jnp.float32), skip_weights[level_index].astype(jnp.float32), precision=lax.Precision.HIGHEST)
        incoming = skip_term + spectral
    return jnp.einsum('cxyz,c->xyz', incoming, lift_weights, precision=lax.Precision.HIGHEST)

def reference(cotangent, pre_activations, spectral_weights, skip_weights, lift_weights):

    def one_sample(sample_index):
        cot_sample = lax.dynamic_index_in_dim(cotangent, sample_index, 0, keepdims=False)
        pre_sample = lax.dynamic_index_in_dim(pre_activations, sample_index, 1, keepdims=False)
        return sample_grad(cot_sample, pre_sample, spectral_weights, skip_weights, lift_weights)
    return lax.map(one_sample, jnp.arange(B, dtype=jnp.int32))
```

```python
import functools
import math

import jax
import jax.numpy as jnp
import numpy as np
from jax import lax
from jax.experimental import pallas as pl
from jax.experimental.pallas import tpu as pltpu
from jax.sharding import PartitionSpec as P

C = 20
NZT = 2048
NA = 16
NB = 8
NG = 3
GC = 7
LM = 36
SCALE_ZT = 1.0 / NZT
BF = jnp.bfloat16
F32 = jnp.float32
INV_SQRT2 = 1.0 / math.sqrt(2.0)
INV_SQRT2PI = 1.0 / math.sqrt(2.0 * math.pi)


def freq(count):
    j = np.arange(count)
    return np.where(j < count // 2, j, j - count)


def plane_table():
    joint = np.arange(24 * 12)
    kz = freq(24)[joint // 12]
    kt = joint % 12
    cell = np.arange(NZT)
    turns = (kz[None, :] * (cell[:, None] // 32) * 32 + kt[None, :] * (cell[:, None] % 32) * 64) % NZT
    angle = 2.0 * np.pi / NZT * turns
    table = np.zeros((NZT, 768))
    owner, local = joint // 18, joint % 18
    column = 128 * (owner // 3) + LM * (owner % 3) + 2 * local
    table[:, column] = np.cos(angle)
    table[:, column + 1] = -np.sin(angle)
    return table


def line_angle():
    return 2.0 * np.pi / 64 * ((freq(24)[:, None] * np.arange(64)[None, :]) % 64)


def x_table():
    angle = line_angle()
    out = np.zeros((2, NB, 4, 8, 64, 8))
    for y in range(8):
        out[0, :, :3, y, :, y] = np.cos(angle).reshape(NB, 3, 64)
        out[1, :, :3, y, :, y] = np.sin(angle).reshape(NB, 3, 64)
    return out.reshape(2, 256, 512)


def y_table():
    angle = line_angle().reshape(24, NB, 8)
    out = np.zeros((2, 80, NB, 4, 8))
    for k in range(3):
        out[0, 24 * k : 24 * k + 24, :, k] = np.cos(angle)
        out[1, 24 * k : 24 * k + 24, :, k] = np.sin(angle)
    return out.reshape(2, 80, 256)


def y_back_table():
    wide = np.zeros((2, 256, 128))
    wide[:, :, :80] = y_table().transpose(0, 2, 1) / 64
    return wide


def swap(values):
    even = lax.broadcasted_iota(jnp.int32, (values.shape[0], 128), 1) % 2 == 0
    parts = []
    for t in range(values.shape[1] // 128):
        part = values[:, 128 * t : 128 * t + 128]
        parts.append(jnp.where(even, pltpu.roll(part, 127, 1), -pltpu.roll(part, 1, 1)))
    return parts[0] if len(parts) == 1 else jnp.concatenate(parts, 1)


def dot(a, b):
    return jnp.dot(a, b, preferred_element_type=F32)


def dot_nt(a, b):
    return lax.dot_general(a, b, (((1,), (1,)), ((), ())), preferred_element_type=F32)


def slope_of(v):
    normal_cdf = 0.5 + 0.5 * lax.erf(v * INV_SQRT2)
    return normal_cdf + v * (jnp.exp(-0.5 * v * v) * INV_SQRT2PI)


def loop(count, body):
    lax.fori_loop(0, count, lambda i, carry: (body(i), carry)[1], 0)


def kernel(
    cot_h, pre_h, wts_h, skip_ref, lift_ref, plane_h, xf_h, xb_h, yf_ref, yb_ref, out_ref,
    cot, pre, wts, plane, xf, xb, g1, g0, slope0, tbuf, bx, kron,
    s1, r1, s2, r2, s3, r3, s4, r4, t1, q1, t2, q2, t3, q3, t4, q4,
    q, sm, mm, mg, mt, weff, fold, fa, vv, mt0, bx0,
    in_sem, send_sem, recv_sem,
):
    me_a = lax.axis_index("aa")
    me_b = lax.axis_index("ba")
    lane = lax.broadcasted_iota(jnp.int32, (8, 128), 1)

    def lanes(rows):
        return lax.broadcasted_iota(jnp.int32, (rows, 128), 1)

    sizes = [min(GC, C - GC * g) for g in range(NG)]
    loads = []
    for g in range(NG):
        part = pl.ds(GC * g, sizes[g])
        loads.append(pltpu.make_async_copy(cot_h.at[part], cot.at[part], in_sem.at[2 * g]))
        loads.append(pltpu.make_async_copy(pre_h.at[1, part], pre.at[1, part], in_sem.at[2 * g + 1]))
    load_plane = pltpu.make_async_copy(plane_h, plane, in_sem.at[6])
    load_pre0 = pltpu.make_async_copy(pre_h.at[0], pre.at[0], in_sem.at[7])
    load_xf = pltpu.make_async_copy(xf_h, xf, in_sem.at[8])
    load_xb = pltpu.make_async_copy(xb_h, xb, in_sem.at[9])
    load_w1 = pltpu.make_async_copy(wts_h.at[1], wts.at[1, :, :, pl.ds(0, C)], in_sem.at[10])
    load_w0 = pltpu.make_async_copy(wts_h.at[0], wts.at[0, :, :, pl.ds(0, C)], in_sem.at[11])
    loads[0].start()
    loads[1].start()
    load_plane.start()
    for copy in loads[2:]:
        copy.start()
    load_xf.start()
    load_pre0.start()
    load_w1.start()
    load_xb.start()
    load_w0.start()

    barrier = pltpu.get_barrier_semaphore()

    def greet_a(d):
        peer = lax.rem(me_a + d + 1, NA)
        pl.semaphore_signal(barrier, 1, device_id={"aa": peer}, device_id_type=pl.DeviceIdType.MESH)

    def greet_b(d):
        peer = lax.rem(me_b + d + 1, NB)
        pl.semaphore_signal(barrier, 1, device_id={"ba": peer}, device_id_type=pl.DeviceIdType.MESH)

    loop(NA - 1, greet_a)
    loop(NB - 1, greet_b)

    g1[C] = jnp.zeros((32, NZT), BF)
    g0[C] = jnp.zeros((32, NZT), BF)
    for level in range(2):
        for k in range(3):
            for p in range(2):
                wts[level, k, p, C] = jnp.zeros((C, 432), BF)
    q[256:296] = jnp.zeros((40, 128), F32)
    mm[...] = jnp.zeros(mm.shape, F32)
    mt[...] = jnp.zeros(mt.shape, F32)
    mt0[...] = jnp.zeros(mt0.shape, F32)
    weff[...] = jnp.zeros(weff.shape, F32)
    fold[...] = jnp.zeros(fold.shape, F32)
    sm[...] = jnp.zeros(sm.shape, F32)

    def send(axis, size, src, dst, slot):
        me = me_a if axis == "aa" else me_b

        def one(d):
            peer = lax.rem(me + d + 1, size)
            pltpu.make_async_remote_copy(
                src_ref=src.at[peer],
                dst_ref=dst.at[me],
                send_sem=send_sem.at[slot],
                recv_sem=recv_sem.at[slot],
                device_id={axis: peer},
                device_id_type=pl.DeviceIdType.MESH,
            ).start()

        loop(size - 1, one)
        dst[me] = src[me]

    def arrive(size, dst, slot):
        part = dst.at[pl.ds(0, size - 1)]
        pltpu.make_async_copy(part, part, recv_sem.at[slot]).wait()

    def drain(size, src, slot):
        part = src.at[pl.ds(0, size - 1)]
        pltpu.make_async_copy(part, part, send_sem.at[slot]).wait()

    def pack(g, dst):
        for a in range(NA):
            t, j = a // 3, a % 3
            for half in range(2):
                low = high = None
                for c in range(GC):
                    piece = tbuf[32 * c + 16 * half : 32 * c + 16 * half + 16, 128 * t : 128 * t + 128]
                    shift = (LM * c - LM * j) % 128
                    if shift:
                        piece = pltpu.roll(piece, shift, 1)
                    start = LM * c
                    if start < 128:
                        low = piece if low is None else jnp.where(lanes(16) < start, low, piece)
                    if start + LM > 128:
                        high = piece if high is None else jnp.where(lanes(16) < start - 128, high, piece)
                dst[g, a, 16 * half : 16 * half + 16, 0:128] = low.astype(BF)
                dst[g, a, 16 * half : 16 * half + 16, 128:256] = high.astype(BF)

    def forward_zt(field, g):
        tbuf[...] = dot(field[pl.ds(GC * g, GC)].reshape(GC * 32, NZT), plane[...])

    def forward_x(src, dst, g):
        values = src[g].reshape(512, 256)
        out = dot(xf[0], values) + swap(dot(xf[1], values))
        dst[g] = out.astype(BF).reshape(NB, 32, 256)

    def forward_y(src, g):
        values = src[g].reshape(256, 256)
        out = dot(yf_ref[0], values) + swap(dot(yf_ref[1], values))
        full = jnp.concatenate([out, jnp.zeros((48, 256), F32)], 0)
        q[0:256] = full.T
        for p in range(2):
            tiles = [[None] * 4 for _ in range(3)]
            for m in range(18):
                rows = q[pl.ds(2 * m + p, 8, stride=LM), :]
                t, off = divmod(24 * m, 128)
                for k in range(3):
                    shift = (24 * m - 24 * k) % 128
                    piece = pltpu.roll(rows, shift, 1) if shift else rows
                    old = tiles[k][t]
                    tiles[k][t] = piece if old is None else jnp.where(lane < off, old, piece)
                    if off + 24 > 128:
                        tiles[k][t + 1] = piece
            for k in range(3):
                for t in range(4):
                    sm[k, p, g, :, 128 * t : 128 * t + 128] = tiles[k][t]

    def mix(g):
        def one(k):
            for t in range(4):
                size = 128 if t < 3 else 48
                part = slice(128 * t, 128 * t + size)
                re = mm[k, 0, 0:C, part]
                im = mm[k, 1, 0:C, part]
                all_re = sm[k, 0, g, :, part]
                all_im = sm[k, 1, g, :, part]
                for c in range(GC):
                    w_re = wts[1, k, 0, GC * g + c, :, part].astype(F32)
                    w_im = wts[1, k, 1, GC * g + c, :, part].astype(F32)
                    s_re = all_re[c : c + 1]
                    s_im = all_im[c : c + 1]
                    re = re + w_re * s_re + w_im * s_im
                    im = im + w_re * s_im - w_im * s_re
                mm[k, 0, 0:C, part] = re
                mm[k, 1, 0:C, part] = im

        loop(3, one)

    def tile_of(load, m):
        t, off = divmod(24 * m, 128)
        value = load(t)
        if off + 24 > 128:
            value = jnp.where(lane < 64, load(t + 1), value)
        return value

    def back_y(dst, g):
        for m in range(18):
            for p in range(2):
                parts = []
                for k in range(3):
                    value = tile_of(lambda t: mg[g, k, p, :, 128 * t : 128 * t + 128], m)
                    shift = (24 * k - 24 * m) % 128
                    parts.append(pltpu.roll(value, shift, 1) if shift else value)
                row = jnp.where(lane < 24, parts[0], jnp.where(lane < 48, parts[1], parts[2]))
                mt[pl.ds(2 * m + p, 8, stride=LM), :] = row
        values = mt[0:256].astype(BF)
        out = dot_nt(yb_ref[0], values) - swap(dot_nt(yb_ref[1], values))
        dst[g] = out.astype(BF).reshape(NB, 32, 256)

    def back_x(values, width):
        turned = -swap(values.astype(F32))
        return dot(xb[0], values) + dot(xb[1], turned.astype(BF))

    def unpack(src, g):
        for half in range(2):
            for c in range(GC):
                start = LM * c
                for t in range(6):
                    parts = []
                    for j in range(3 if t < 5 else 1):
                        a = 3 * t + j
                        rows = slice(16 * half, 16 * half + 16)
                        low = start // 128
                        value = src[g, a, rows, 128 * low : 128 * low + 128].astype(F32)
                        if start % 128 + LM > 128:
                            other = src[g, a, rows, 128:256].astype(F32)
                            value = jnp.where(lanes(16) < 64, other, value)
                        shift = (LM * j - start) % 128
                        parts.append(pltpu.roll(value, shift, 1) if shift else value)
                    full = parts[0]
                    for j in range(1, len(parts)):
                        full = jnp.where(lanes(16) < LM * j, full, parts[j])
                    bx[32 * c + 16 * half : 32 * c + 16 * half + 16, 128 * t : 128 * t + 128] = full.astype(BF)

    def grad_top(g):
        def one(i):
            c = GC * g + i
            for pair in range(2):
                for n in range(4):
                    part = slice(512 * n, 512 * n + 512)
                    v = pre[1, c, 2 * pair : 2 * pair + 2, :, part].astype(F32).reshape(16, 512)
                    d = cot[c, 2 * pair : 2 * pair + 2, :, part].astype(F32).reshape(16, 512)
                    g1[c, 16 * pair : 16 * pair + 16, part] = (d * slope_of(v)).astype(BF)

        loop(sizes[g], one)

    for g in range(NG):
        loads[2 * g].wait()
        loads[2 * g + 1].wait()
        grad_top(g)
        if g == 0:
            load_plane.wait()
        forward_zt(g1, g)
        pack(g, s1)
        if g == 0:
            pl.semaphore_wait(barrier, NA + NB - 2)
        send("aa", NA, s1.at[g], r1.at[g], g)

    def spread(rows, groups):
        r = lax.broadcasted_iota(jnp.int32, (rows, groups), 0) // 16
        return (r == lax.broadcasted_iota(jnp.int32, (rows, groups), 1)).astype(BF)

    left = dot_nt(spread(336, C), skip_ref[1]).astype(BF)
    wide = dot_nt(left, spread(320, C))
    same = lax.broadcasted_iota(jnp.int32, (336, 320), 0) % 16 == lax.broadcasted_iota(jnp.int32, (336, 320), 1) % 16
    kron[...] = jnp.where(same, wide, 0.0).astype(BF)

    load_xf.wait()

    def stage_x1(g):
        arrive(NA, r1.at[g], g)
        forward_x(r1, s2, g)
        send("ba", NB, s2.at[g], r2.at[g], 3 + g)

    loop(NG, stage_x1)

    load_pre0.wait()

    def slope_one(c):
        for pair in range(2):
            for n in range(4):
                part = slice(512 * n, 512 * n + 512)
                v = pre[0, c, 2 * pair : 2 * pair + 2, :, part].astype(F32).reshape(16, 512)
                slope0[c, 16 * pair : 16 * pair + 16, part] = slope_of(v)

    loop(C, slope_one)

    load_w1.wait()

    def stage_y1(g):
        arrive(NB, r2.at[g], 3 + g)
        forward_y(r2, g)
        mix(g)

    loop(NG, stage_y1)
    for g in range(NG):
        for k in range(3):
            for p in range(2):
                mg[g, k, p] = mm[k, p, GC * g : GC * g + 8, :]

    def stage_yb(g):
        back_y(s3, g)
        send("ba", NB, s3.at[g], r3.at[g], 6 + g)

    loop(NG, stage_yb)
    load_xb.wait()

    def stage_xb(g):
        arrive(NB, r3.at[g], 6 + g)
        out = back_x(r3[g].reshape(256, 256), 256)
        s4[g] = out.astype(BF).reshape(NA, 32, 256)
        send("aa", NA, s4.at[g], r4.at[g], 9 + g)

    loop(NG, stage_xb)

    load_w0.wait()
    lift_col = lift_ref[...]

    def fold_weights(i):
        k = i // 2
        p = lax.rem(i, 2)

        def inner(g):
            for c in range(GC):
                row = jnp.sum(wts[0, k, p, GC * g + c].astype(F32) * lift_col, 0, keepdims=True)
                weff[k, p, g, c : c + 1, 0:432] = row

        loop(NG, inner)

    loop(6, fold_weights)

    def stage_field(g):
        arrive(NA, r4.at[g], 9 + g)
        unpack(r4, g)

        def piece(n):
            part = pl.ds(pl.multiple_of(512 * n, 512), 512)
            spectral = dot_nt(bx[...], plane[part, :])
            spectral = spectral.reshape(GC, 2, 16, 512)
            for pair in range(2):
                skip = dot(
                    kron[pl.ds(112 * g, 112), :],
                    g1[0:C, 16 * pair : 16 * pair + 16, part].reshape(320, 512),
                ).reshape(GC, 16, 512)
                incoming = skip + spectral[:, pair] * SCALE_ZT
                for c in range(GC):
                    slope = slope0[jnp.minimum(GC * g + c, C - 1), 16 * pair : 16 * pair + 16, part]
                    g0[GC * g + c, 16 * pair : 16 * pair + 16, part] = (incoming[c] * slope).astype(BF)

        loop(4, piece)
        forward_zt(g0, g)
        pack(g, t1)
        send("aa", NA, t1.at[g], q1.at[g], 12 + g)

    loop(NG, stage_field)

    def stage_x0(g):
        arrive(NA, q1.at[g], 12 + g)
        forward_x(q1, t2, g)
        send("ba", NB, t2.at[g], q2.at[g], 15 + g)

    loop(NG, stage_x0)

    gain = jnp.sum(skip_ref[0].astype(F32) * lift_ref[...].reshape(1, C), 1, keepdims=True)

    def skip_piece(n):
        part = pl.ds(pl.multiple_of(512 * n, 512), 512)
        for pair in range(2):
            rows = slice(16 * pair, 16 * pair + 16)
            total = jnp.zeros((16, 512), F32)
            for c in range(C):
                total = total + g0[c, rows, part].astype(F32) * gain[c : c + 1, :]
            out_ref[rows, part] = total

    loop(4, skip_piece)

    def stage_y0(g):
        arrive(NB, q2.at[g], 15 + g)
        forward_y(q2, g)
        for k in range(3):
            w_re, w_im = weff[k, 0, g], weff[k, 1, g]
            s_re, s_im = sm[k, 0, g], sm[k, 1, g]
            fold[k] += w_re * s_re + w_im * s_im
            fold[3 + k] += w_re * s_im - w_im * s_re

    loop(NG, stage_y0)

    for i in range(6):
        fa[i : i + 1] = jnp.sum(fold[i], 0, keepdims=True)
    fa[6:8] = jnp.zeros((2, 512), F32)
    for m in range(18):
        value = tile_of(lambda t: fa[:, 128 * t : 128 * t + 128], m)
        shift = (-24 * m) % 128
        vv[8 * m : 8 * m + 8] = pltpu.roll(value, shift, 1) if shift else value
    for p in range(2):
        parts = []
        for k in range(3):
            value = vv[pl.ds(3 * p + k, 18, stride=8), :]
            parts.append(pltpu.roll(value, 24 * k, 1) if k else value)
        full = jnp.where(lanes(18) < 24, parts[0], jnp.where(lanes(18) < 48, parts[1], parts[2]))
        mt0[pl.ds(p, 18, stride=2), :] = full
    values = mt0[...].astype(BF)
    out = dot_nt(yb_ref[0], values) - swap(dot_nt(yb_ref[1], values))
    t3[...] = out.astype(BF).reshape(NB, 32, 128)
    send("ba", NB, t3, q3, 18)
    arrive(NB, q3, 18)
    t4[...] = back_x(q3[...].reshape(256, 128), 128).astype(BF).reshape(NA, 32, 128)
    send("aa", NA, t4, q4, 19)
    arrive(NA, q4, 19)
    for t in range(6):
        full = None
        for j in range(3 if t < 5 else 1):
            value = q4[3 * t + j].astype(F32)
            if j:
                value = jnp.where(lanes(32) < LM * j, full, pltpu.roll(value, LM * j, 1))
            full = value
        bx0[:, 128 * t : 128 * t + 128] = full.astype(BF)

    def last(n):
        part = pl.ds(pl.multiple_of(512 * n, 512), 512)
        out_ref[:, part] += dot_nt(bx0[...], plane[part, :]) * SCALE_ZT

    loop(4, last)

    for g in range(NG):
        drain(NA, s1.at[g], g)
        drain(NB, s2.at[g], 3 + g)
        drain(NB, s3.at[g], 6 + g)
        drain(NA, s4.at[g], 9 + g)
        drain(NA, t1.at[g], 12 + g)
        drain(NB, t2.at[g], 15 + g)
    drain(NB, t3, 18)
    drain(NA, t4, 19)


def per_device(cotangent, pre_activations, spectral_weights, skip_weights, lift_weights):
    bf = lambda table: jnp.asarray(table.astype(np.float32), dtype=BF)
    forward_x_table = x_table()
    back_x_table = forward_x_table.transpose(0, 2, 1) / 64
    any_spec = pl.BlockSpec(memory_space=pl.ANY)
    vmem_spec = pl.BlockSpec(memory_space=pltpu.VMEM)
    block_a, block_b = (NG, NA, 32, 256), (NG, NB, 32, 256)
    scratch = [
        pltpu.VMEM((C, 4, 8, NZT), BF),
        pltpu.VMEM((2, C, 4, 8, NZT), BF),
        pltpu.VMEM((2, 3, 2, C + 1, C, 432), BF),
        pltpu.VMEM((NZT, 768), BF),
        pltpu.VMEM((2, 256, 512), BF),
        pltpu.VMEM((2, 512, 256), BF),
        pltpu.VMEM((C + 1, 32, NZT), BF),
        pltpu.VMEM((C + 1, 32, NZT), BF),
        pltpu.VMEM((C, 32, NZT), F32),
        pltpu.VMEM((224, 768), F32),
        pltpu.VMEM((224, 768), BF),
        pltpu.VMEM((336, 320), BF),
        pltpu.VMEM(block_a, BF), pltpu.VMEM(block_a, BF),
        pltpu.VMEM(block_b, BF), pltpu.VMEM(block_b, BF),
        pltpu.VMEM(block_b, BF), pltpu.VMEM(block_b, BF),
        pltpu.VMEM(block_a, BF), pltpu.VMEM(block_a, BF),
        pltpu.VMEM(block_a, BF), pltpu.VMEM(block_a, BF),
        pltpu.VMEM(block_b, BF), pltpu.VMEM(block_b, BF),
        pltpu.VMEM((NB, 32, 128), BF), pltpu.VMEM((NB, 32, 128), BF),
        pltpu.VMEM((NA, 32, 128), BF), pltpu.VMEM((NA, 32, 128), BF),
        pltpu.VMEM((296, 128), F32),
        pltpu.VMEM((3, 2, NG, 8, 512), F32),
        pltpu.VMEM((3, 2, 24, 512), F32),
        pltpu.VMEM((NG, 3, 2, 8, 512), F32),
        pltpu.VMEM((296, 128), F32),
        pltpu.VMEM((3, 2, NG, 8, 512), F32),
        pltpu.VMEM((6, 8, 512), F32),
        pltpu.VMEM((8, 512), F32),
        pltpu.VMEM((144, 128), F32),
        pltpu.VMEM((128, 128), F32),
        pltpu.VMEM((32, 768), BF),
        pltpu.SemaphoreType.DMA((12,)),
        pltpu.SemaphoreType.DMA((20,)),
        pltpu.SemaphoreType.DMA((20,)),
    ]
    out = pl.pallas_call(
        kernel,
        out_shape=jax.ShapeDtypeStruct((32, NZT), F32),
        in_specs=[any_spec] * 3 + [vmem_spec] * 2 + [any_spec] * 3 + [vmem_spec] * 2,
        out_specs=vmem_spec,
        scratch_shapes=scratch,
        compiler_params=pltpu.CompilerParams(
            collective_id=0, has_side_effects=True, vmem_limit_bytes=64000000
        ),
        name="fno_grad",
    )(
        cotangent.reshape(C, 4, 8, NZT),
        pre_activations.reshape(2, C, 4, 8, NZT),
        spectral_weights.transpose(0, 4, 1, 2, 3, 5),
        skip_weights,
        lift_weights.reshape(C, 1),
        bf(plane_table()),
        bf(forward_x_table),
        bf(back_x_table),
        bf(y_table()),
        bf(y_back_table()),
    )
    return out.reshape(1, 4, 8, NZT)


def solution(mesh):
    return jax.shard_map(
        per_device,
        mesh=mesh,
        in_specs=(
            P(None, None, "aa", "ba", None),
            P(None, None, None, "aa", "ba", None),
            P(None, None, None, None, "ba", "aa"),
            P(),
            P(),
        ),
        out_specs=P(None, "aa", "ba", None),
        check_vma=False,
    )
```

```python
import functools
import math

import jax
import jax.numpy as jnp
import numpy as np
from jax import lax
from jax.experimental import pallas as pl
from jax.experimental.pallas import tpu as pltpu
from jax.sharding import PartitionSpec as P

C = 20
NZT = 2048
NA = 16
NB = 8
NG = 3
GC = 7
LM = 36
SCALE_ZT = 1.0 / NZT
BF = jnp.bfloat16
F32 = jnp.float32
INV_SQRT2 = 1.0 / math.sqrt(2.0)
INV_SQRT2PI = 1.0 / math.sqrt(2.0 * math.pi)


def freq(count):
    j = np.arange(count)
    return np.where(j < count // 2, j, j - count)


def plane_table():
    joint = np.arange(24 * 12)
    kz = freq(24)[joint // 12]
    kt = joint % 12
    cell = np.arange(NZT)
    turns = (kz[None, :] * (cell[:, None] // 32) * 32 + kt[None, :] * (cell[:, None] % 32) * 64) % NZT
    angle = 2.0 * np.pi / NZT * turns
    table = np.zeros((NZT, 768))
    owner, local = joint // 18, joint % 18
    column = 128 * (owner // 3) + LM * (owner % 3) + 2 * local
    table[:, column] = np.cos(angle)
    table[:, column + 1] = -np.sin(angle)
    return table


def line_angle():
    return 2.0 * np.pi / 64 * ((freq(24)[:, None] * np.arange(64)[None, :]) % 64)


def x_table():
    angle = line_angle()
    out = np.zeros((2, NB, 4, 8, 64, 8))
    for y in range(8):
        out[0, :, :3, y, :, y] = np.cos(angle).reshape(NB, 3, 64)
        out[1, :, :3, y, :, y] = np.sin(angle).reshape(NB, 3, 64)
    return out.reshape(2, 256, 512)


def y_table():
    angle = line_angle().reshape(24, NB, 8)
    out = np.zeros((2, 80, NB, 4, 8))
    for k in range(3):
        out[0, 24 * k : 24 * k + 24, :, k] = np.cos(angle)
        out[1, 24 * k : 24 * k + 24, :, k] = np.sin(angle)
    return out.reshape(2, 80, 256)


def y_back_table():
    wide = np.zeros((2, 256, 128))
    wide[:, :, :80] = y_table().transpose(0, 2, 1) / 64
    return wide


def swap(values):
    even = lax.broadcasted_iota(jnp.int32, (values.shape[0], 128), 1) % 2 == 0
    parts = []
    for t in range(values.shape[1] // 128):
        part = values[:, 128 * t : 128 * t + 128]
        parts.append(jnp.where(even, pltpu.roll(part, 127, 1), -pltpu.roll(part, 1, 1)))
    return parts[0] if len(parts) == 1 else jnp.concatenate(parts, 1)


def dot(a, b):
    return jnp.dot(a, b, preferred_element_type=F32)


def dot_nt(a, b):
    return lax.dot_general(a, b, (((1,), (1,)), ((), ())), preferred_element_type=F32)


def slope_of(v):
    normal_cdf = 0.5 + 0.5 * lax.erf(v * INV_SQRT2)
    return normal_cdf + v * (jnp.exp(-0.5 * v * v) * INV_SQRT2PI)


def loop(count, body):
    lax.fori_loop(0, count, lambda i, carry: (body(i), carry)[1], 0)


def kernel(
    cot_h, pre_h, wts_h, skip_ref, lift_s, lift_ref, plane_h, xf_h, xb_h, yf_ref, yb_ref, out_ref,
    cot, pre, wts, plane, xf, xb, g1, g0, slope0, skip1, tbuf, bx, kron, wide,
    s1, r1, s2, r2, s3, r3, s4, r4, t1, q1, t2, q2, t3, q3, t4, q4,
    q, sm, mm, mg, mt, weff, fold, fa, vv, mt0, bx0,
    in_sem, send_sem, recv_sem,
):
    me_a = lax.axis_index("aa")
    me_b = lax.axis_index("ba")
    lane = lax.broadcasted_iota(jnp.int32, (8, 128), 1)

    def lanes(rows):
        return lax.broadcasted_iota(jnp.int32, (rows, 128), 1)

    sizes = [min(GC, C - GC * g) for g in range(NG)]
    loads = []
    for g in range(NG):
        part = pl.ds(GC * g, sizes[g])
        loads.append(pltpu.make_async_copy(cot_h.at[part], cot.at[part], in_sem.at[2 * g]))
        loads.append(pltpu.make_async_copy(pre_h.at[1, part], pre.at[1, part], in_sem.at[2 * g + 1]))
    load_plane = pltpu.make_async_copy(plane_h, plane, in_sem.at[6])
    load_pre0 = pltpu.make_async_copy(pre_h.at[0], pre.at[0], in_sem.at[7])
    load_xf = pltpu.make_async_copy(xf_h, xf, in_sem.at[8])
    load_xb = pltpu.make_async_copy(xb_h, xb, in_sem.at[9])
    load_w1 = pltpu.make_async_copy(wts_h.at[1], wts.at[1], in_sem.at[10])
    load_w0 = pltpu.make_async_copy(wts_h.at[0], wts.at[0], in_sem.at[11])
    loads[0].start()
    loads[1].start()
    load_plane.start()

    barrier = pltpu.get_barrier_semaphore()

    def greet_a(d):
        peer = lax.rem(me_a + d + 1, NA)
        pl.semaphore_signal(barrier, 1, device_id={"aa": peer}, device_id_type=pl.DeviceIdType.MESH)

    def greet_b(d):
        peer = lax.rem(me_b + d + 1, NB)
        pl.semaphore_signal(barrier, 1, device_id={"ba": peer}, device_id_type=pl.DeviceIdType.MESH)

    loop(NA - 1, greet_a)
    loop(NB - 1, greet_b)

    g1[C] = jnp.zeros((32, NZT), BF)
    g0[C] = jnp.zeros((32, NZT), BF)
    for k in range(3):
        wide[C, k] = jnp.zeros((40, 432), F32)
    for box in (r2, r3, q2, q3):
        box[..., 24:32, :] = jnp.zeros(box.shape[:-2] + (8, box.shape[-1]), BF)
    q[256:296] = jnp.zeros((40, 128), F32)
    mm[...] = jnp.zeros(mm.shape, F32)
    mt[...] = jnp.zeros(mt.shape, F32)
    mt0[...] = jnp.zeros(mt0.shape, F32)
    weff[...] = jnp.zeros(weff.shape, F32)
    fold[...] = jnp.zeros(fold.shape, F32)
    sm[...] = jnp.zeros(sm.shape, F32)

    def partners(axis):
        if axis == "aa":
            order = [
                (1, 2, 0), (1, 2, 1), (1, 1, 0), (1, 3, 0), (1, 1, 1), (1, 3, 1), (1, 0, 0), (1, 0, 1),
                (0, 2, 0), (0, 2, 1), (0, 1, 0), (0, 3, 0), (0, 1, 1), (0, 3, 1), (0, 0, 1),
            ]
            z, x, core = me_a // 8, lax.rem(me_a // 2, 4), lax.rem(me_a, 2)
            return [
                lax.rem(z + dz, 2) * 8 + lax.rem(x + dx, 4) * 2 + lax.rem(core + dc, 2)
                for dz, dx, dc in order
            ]
        z, y = me_b // 4, lax.rem(me_b, 4)
        order = [(1, 2), (0, 2), (1, 1), (1, 3), (0, 1), (0, 3), (1, 0)]
        return [lax.rem(z + dz, 2) * 4 + lax.rem(y + dy, 4) for dz, dy in order]

    def send(axis, src, dst, slot):
        me = me_a if axis == "aa" else me_b
        rows = pl.ds(0, 32 if axis == "aa" else 24)
        for peer in partners(axis):
            pltpu.make_async_remote_copy(
                src_ref=src.at[peer, rows],
                dst_ref=dst.at[me, rows],
                send_sem=send_sem.at[slot],
                recv_sem=recv_sem.at[slot],
                device_id={axis: peer},
                device_id_type=pl.DeviceIdType.MESH,
            ).start()
        dst[me] = src[me]

    def span(axis, box):
        if axis == "aa":
            return box.at[pl.ds(0, NA - 1)]
        return box.at[pl.ds(0, NB - 1), pl.ds(0, 24)]

    def arrive(axis, dst, slot):
        part = span(axis, dst)
        pltpu.make_async_copy(part, part, recv_sem.at[slot]).wait()

    def drain(axis, src, slot):
        part = span(axis, src)
        pltpu.make_async_copy(part, part, send_sem.at[slot]).wait()

    def pack(g, dst):
        for a in range(NA):
            t, j = a // 3, a % 3
            for half in range(2):
                low = high = None
                for c in range(GC):
                    piece = tbuf[32 * c + 16 * half : 32 * c + 16 * half + 16, 128 * t : 128 * t + 128]
                    shift = (LM * c - LM * j) % 128
                    if shift:
                        piece = pltpu.roll(piece, shift, 1)
                    start = LM * c
                    if start < 128:
                        low = piece if low is None else jnp.where(lanes(16) < start, low, piece)
                    if start + LM > 128:
                        high = piece if high is None else jnp.where(lanes(16) < start - 128, high, piece)
                dst[g, a, 16 * half : 16 * half + 16, 0:128] = low.astype(BF)
                dst[g, a, 16 * half : 16 * half + 16, 128:256] = high.astype(BF)

    def forward_zt(field, g):
        tbuf[...] = dot(field[pl.ds(GC * g, GC)].reshape(GC * 32, NZT), plane[...])

    def forward_x(src, dst, g):
        values = src[g].reshape(512, 256)
        out = dot(xf[0], values) + swap(dot(xf[1], values))
        dst[g] = out.astype(BF).reshape(NB, 32, 256)

    def forward_y(src, g):
        values = src[g].reshape(256, 256)
        out = dot(yf_ref[0], values) + swap(dot(yf_ref[1], values))
        full = jnp.concatenate([out, jnp.zeros((48, 256), F32)], 0)
        q[0:256] = full.T
        for p in range(2):
            tiles = [[None] * 4 for _ in range(3)]
            for m in range(18):
                rows = q[pl.ds(2 * m + p, 8, stride=LM), :]
                t, off = divmod(24 * m, 128)
                for k in range(3):
                    shift = (24 * m - 24 * k) % 128
                    piece = pltpu.roll(rows, shift, 1) if shift else rows
                    old = tiles[k][t]
                    tiles[k][t] = piece if old is None else jnp.where(lane < off, old, piece)
                    if off + 24 > 128:
                        tiles[k][t + 1] = piece
            for k in range(3):
                for t in range(4):
                    sm[k, p, g, :, 128 * t : 128 * t + 128] = tiles[k][t]

    def mix(g):
        def one(k):
            for t in range(4):
                size = 128 if t < 3 else 48
                part = slice(128 * t, 128 * t + size)
                by_re = mm[k, 0, t, 0:40, 0:size]
                by_im = mm[k, 1, t, 0:40, 0:size]
                all_re = sm[k, 0, g, :, part]
                all_im = sm[k, 1, g, :, part]
                for c in range(GC):
                    w = wide[GC * g + c, k, :, part]
                    by_re = by_re + w * all_re[c : c + 1]
                    by_im = by_im + w * all_im[c : c + 1]
                mm[k, 0, t, 0:40, 0:size] = by_re
                mm[k, 1, t, 0:40, 0:size] = by_im

        loop(3, one)

    def unmix(g):
        first, second = pl.ds(2 * GC * g, 8, stride=2), pl.ds(2 * GC * g + 1, 8, stride=2)
        for k in range(3):
            for t in range(4):
                part = slice(128 * t, 128 * t + 128)
                mg[g, k, 0, :, part] = mm[k, 0, t, first, :] + mm[k, 1, t, second, :]
                mg[g, k, 1, :, part] = mm[k, 1, t, first, :] - mm[k, 0, t, second, :]

    def tile_of(load, m):
        t, off = divmod(24 * m, 128)
        value = load(t)
        if off + 24 > 128:
            value = jnp.where(lane < 64, load(t + 1), value)
        return value

    def back_y(dst, g):
        for m in range(18):
            for p in range(2):
                parts = []
                for k in range(3):
                    value = tile_of(lambda t: mg[g, k, p, :, 128 * t : 128 * t + 128], m)
                    shift = (24 * k - 24 * m) % 128
                    parts.append(pltpu.roll(value, shift, 1) if shift else value)
                row = jnp.where(lane < 24, parts[0], jnp.where(lane < 48, parts[1], parts[2]))
                mt[pl.ds(2 * m + p, 8, stride=LM), :] = row
        values = mt[0:256].astype(BF)
        out = dot_nt(yb_ref[0], values) - swap(dot_nt(yb_ref[1], values))
        dst[g] = out.astype(BF).reshape(NB, 32, 256)

    def back_x(values, width):
        turned = -swap(values.astype(F32))
        return dot(xb[0], values) + dot(xb[1], turned.astype(BF))

    def unpack(src, g):
        for half in range(2):
            for c in range(GC):
                start = LM * c
                for t in range(6):
                    parts = []
                    for j in range(3 if t < 5 else 1):
                        a = 3 * t + j
                        rows = slice(16 * half, 16 * half + 16)
                        low = start // 128
                        value = src[g, a, rows, 128 * low : 128 * low + 128].astype(F32)
                        if start % 128 + LM > 128:
                            other = src[g, a, rows, 128:256].astype(F32)
                            value = jnp.where(lanes(16) < 64, other, value)
                        shift = (LM * j - start) % 128
                        parts.append(pltpu.roll(value, shift, 1) if shift else value)
                    full = parts[0]
                    for j in range(1, len(parts)):
                        full = jnp.where(lanes(16) < LM * j, full, parts[j])
                    bx[32 * c + 16 * half : 32 * c + 16 * half + 16, 128 * t : 128 * t + 128] = full.astype(BF)

    def grad_top(g):
        def one(i):
            c = GC * g + i
            for pair in range(2):
                for n in range(4):
                    part = slice(512 * n, 512 * n + 512)
                    v = pre[1, c, 2 * pair : 2 * pair + 2, :, part].astype(F32).reshape(16, 512)
                    d = cot[c, 2 * pair : 2 * pair + 2, :, part].astype(F32).reshape(16, 512)
                    g1[c, 16 * pair : 16 * pair + 16, part] = (d * slope_of(v)).astype(BF)

        loop(sizes[g], one)

    for g in range(NG):
        loads[2 * g].wait()
        loads[2 * g + 1].wait()
        grad_top(g)
        if g == 0:
            load_plane.wait()
            for copy in loads[2:] + [load_w1, load_xf, load_pre0, load_xb, load_w0]:
                copy.start()
        forward_zt(g1, g)
        pack(g, s1)
        if g == 0:
            pl.semaphore_wait(barrier, NA + NB - 2)
        send("aa", s1.at[g], r1.at[g], g)

    def spread(rows, groups):
        r = lax.broadcasted_iota(jnp.int32, (rows, groups), 0) // 16
        return (r == lax.broadcasted_iota(jnp.int32, (rows, groups), 1)).astype(BF)

    skip_all = skip_ref[...].astype(F32)
    left = dot_nt(spread(320, C), skip_all[:, 1, :].astype(BF)).astype(BF)
    whole = dot_nt(left, spread(320, C))
    same = lax.broadcasted_iota(jnp.int32, (320, 320), 0) % 16 == lax.broadcasted_iota(jnp.int32, (320, 320), 1) % 16
    kron[...] = jnp.where(same, whole, 0.0).astype(BF)

    load_w1.wait()

    def widen(o):
        for k in range(3):
            for t in range(4):
                part = slice(128 * t, min(128 * t + 128, 432))
                wide[o, k, :, part] = wts[1, o, :, k, :, part].reshape(40, part.stop - part.start).astype(F32)

    loop(C, widen)
    load_xf.wait()

    def stage_x1(g):
        arrive("aa", r1.at[g], g)
        forward_x(r1, s2, g)
        send("ba", s2.at[g], r2.at[g], 3 + g)

    stage_x1(0)

    def skip_piece1(n):
        part = pl.ds(pl.multiple_of(512 * n, 512), 512)
        for pair in range(2):
            rows = slice(16 * pair, 16 * pair + 16)
            out = dot(kron[...], g1[0:C, rows, part].reshape(320, 512))
            skip1[:, rows, part] = out.reshape(C, 16, 512)

    loop(4, skip_piece1)
    stage_x1(1)
    stage_x1(2)

    def stage_y1(g):
        arrive("ba", r2.at[g], 3 + g)
        forward_y(r2, g)
        mix(g)

    loop(NG, stage_y1)
    for g in range(NG):
        unmix(g)

    def stage_yb(g):
        back_y(s3, g)
        send("ba", s3.at[g], r3.at[g], 6 + g)

    loop(NG, stage_yb)
    load_w0.wait()

    def fold_weights(i):
        k = i // NG
        g = lax.rem(i, NG)
        for c in range(GC):
            o = jnp.minimum(GC * g + c, C - 1)
            for t in range(4):
                part = slice(128 * t, min(128 * t + 128, 432))
                total = wts[0, o, 0, k, :, part].astype(F32) * lift_s[0]
                for i in range(1, C):
                    total = total + wts[0, o, i, k, :, part].astype(F32) * lift_s[i]
                weff[k, 0, g, c : c + 1, part] = total[0:1]
                weff[k, 1, g, c : c + 1, part] = total[1:2]

    loop(9, fold_weights)
    for k in range(3):
        for p in range(2):
            weff[k, p, 2, 6:7] = jnp.zeros((1, 512), F32)

    load_xb.wait()

    def stage_xb(g):
        arrive("ba", r3.at[g], 6 + g)
        out = back_x(r3[g].reshape(256, 256), 256)
        s4[g] = out.astype(BF).reshape(NA, 32, 256)
        send("aa", s4.at[g], r4.at[g], 9 + g)

    loop(NG, stage_xb)

    load_pre0.wait()

    def slope_one(c):
        for pair in range(2):
            for n in range(4):
                part = slice(512 * n, 512 * n + 512)
                v = pre[0, c, 2 * pair : 2 * pair + 2, :, part].astype(F32).reshape(16, 512)
                slope0[c, 16 * pair : 16 * pair + 16, part] = slope_of(v)

    loop(C, slope_one)

    def stage_field(g):
        arrive("aa", r4.at[g], 9 + g)
        unpack(r4, g)

        def piece(n):
            part = pl.ds(pl.multiple_of(512 * n, 512), 512)
            spectral = dot_nt(bx[...], plane[part, :])
            spectral = spectral.reshape(GC, 2, 16, 512)
            for pair in range(2):
                rows = slice(16 * pair, 16 * pair + 16)
                for c in range(GC):
                    o = jnp.minimum(GC * g + c, C - 1)
                    incoming = skip1[o, rows, part] + spectral[c, pair] * SCALE_ZT
                    g0[GC * g + c, rows, part] = (incoming * slope0[o, rows, part]).astype(BF)

        loop(4, piece)
        forward_zt(g0, g)
        pack(g, t1)
        send("aa", t1.at[g], q1.at[g], 12 + g)

    loop(NG, stage_field)

    def stage_x0(g):
        arrive("aa", q1.at[g], 12 + g)
        forward_x(q1, t2, g)
        send("ba", t2.at[g], q2.at[g], 15 + g)

    loop(NG, stage_x0)

    gain = jnp.sum(skip_all[:, 0, :] * lift_ref[...], 1, keepdims=True)

    def skip_piece(n):
        part = pl.ds(pl.multiple_of(512 * n, 512), 512)
        for pair in range(2):
            rows = slice(16 * pair, 16 * pair + 16)
            total = jnp.zeros((16, 512), F32)
            for c in range(C):
                total = total + g0[c, rows, part].astype(F32) * gain[c : c + 1, :]
            out_ref[rows, part] = total

    loop(4, skip_piece)

    def stage_y0(g):
        arrive("ba", q2.at[g], 15 + g)
        forward_y(q2, g)
        for k in range(3):
            w_re, w_im = weff[k, 0, g], weff[k, 1, g]
            s_re, s_im = sm[k, 0, g], sm[k, 1, g]
            fold[k] += w_re * s_re + w_im * s_im
            fold[3 + k] += w_re * s_im - w_im * s_re

    loop(NG, stage_y0)

    for i in range(6):
        fa[i : i + 1] = jnp.sum(fold[i], 0, keepdims=True)
    fa[6:8] = jnp.zeros((2, 512), F32)
    for m in range(18):
        value = tile_of(lambda t: fa[:, 128 * t : 128 * t + 128], m)
        shift = (-24 * m) % 128
        vv[8 * m : 8 * m + 8] = pltpu.roll(value, shift, 1) if shift else value
    for p in range(2):
        parts = []
        for k in range(3):
            value = vv[pl.ds(3 * p + k, 18, stride=8), :]
            parts.append(pltpu.roll(value, 24 * k, 1) if k else value)
        full = jnp.where(lanes(18) < 24, parts[0], jnp.where(lanes(18) < 48, parts[1], parts[2]))
        mt0[pl.ds(p, 18, stride=2), :] = full
    values = mt0[...].astype(BF)
    out = dot_nt(yb_ref[0], values) - swap(dot_nt(yb_ref[1], values))
    t3[...] = out.astype(BF).reshape(NB, 32, 128)
    send("ba", t3, q3, 18)
    arrive("ba", q3, 18)
    t4[...] = back_x(q3[...].reshape(256, 128), 128).astype(BF).reshape(NA, 32, 128)
    send("aa", t4, q4, 19)
    arrive("aa", q4, 19)
    for t in range(6):
        full = None
        for j in range(3 if t < 5 else 1):
            value = q4[3 * t + j].astype(F32)
            if j:
                value = jnp.where(lanes(32) < LM * j, full, pltpu.roll(value, LM * j, 1))
            full = value
        bx0[:, 128 * t : 128 * t + 128] = full.astype(BF)

    def last(n):
        part = pl.ds(pl.multiple_of(512 * n, 512), 512)
        out_ref[:, part] += dot_nt(bx0[...], plane[part, :]) * SCALE_ZT

    loop(4, last)

    for g in range(NG):
        drain("aa", s1.at[g], g)
        drain("ba", s2.at[g], 3 + g)
        drain("ba", s3.at[g], 6 + g)
        drain("aa", s4.at[g], 9 + g)
        drain("aa", t1.at[g], 12 + g)
        drain("ba", t2.at[g], 15 + g)
    drain("ba", t3, 18)
    drain("aa", t4, 19)


def per_device(cotangent, pre_activations, spectral_weights, skip_weights, lift_weights):
    bf = lambda table: jnp.asarray(table.astype(np.float32), dtype=BF)
    forward_x_table = x_table()
    back_x_table = forward_x_table.transpose(0, 2, 1) / 64
    any_spec = pl.BlockSpec(memory_space=pl.ANY)
    vmem_spec = pl.BlockSpec(memory_space=pltpu.VMEM)
    smem_spec = pl.BlockSpec(memory_space=pltpu.SMEM)
    block_a, block_b = (NG, NA, 32, 256), (NG, NB, 32, 256)
    scratch = [
        pltpu.VMEM((C, 4, 8, NZT), BF),
        pltpu.VMEM((2, C, 4, 8, NZT), BF),
        pltpu.VMEM((2, C, C, 3, 2, 432), BF),
        pltpu.VMEM((NZT, 768), BF),
        pltpu.VMEM((2, 256, 512), BF),
        pltpu.VMEM((2, 512, 256), BF),
        pltpu.VMEM((C + 1, 32, NZT), BF),
        pltpu.VMEM((C + 1, 32, NZT), BF),
        pltpu.VMEM((C, 32, NZT), F32),
        pltpu.VMEM((C, 32, NZT), F32),
        pltpu.VMEM((224, 768), F32),
        pltpu.VMEM((224, 768), BF),
        pltpu.VMEM((320, 320), BF),
        pltpu.VMEM((C + 1, 3, 40, 432), F32),
        pltpu.VMEM(block_a, BF), pltpu.VMEM(block_a, BF),
        pltpu.VMEM(block_b, BF), pltpu.VMEM(block_b, BF),
        pltpu.VMEM(block_b, BF), pltpu.VMEM(block_b, BF),
        pltpu.VMEM(block_a, BF), pltpu.VMEM(block_a, BF),
        pltpu.VMEM(block_a, BF), pltpu.VMEM(block_a, BF),
        pltpu.VMEM(block_b, BF), pltpu.VMEM(block_b, BF),
        pltpu.VMEM((NB, 32, 128), BF), pltpu.VMEM((NB, 32, 128), BF),
        pltpu.VMEM((NA, 32, 128), BF), pltpu.VMEM((NA, 32, 128), BF),
        pltpu.VMEM((296, 128), F32),
        pltpu.VMEM((3, 2, NG, 8, 512), F32),
        pltpu.VMEM((3, 2, 4, 48, 128), F32),
        pltpu.VMEM((NG, 3, 2, 8, 512), F32),
        pltpu.VMEM((296, 128), F32),
        pltpu.VMEM((3, 2, NG, 8, 512), F32),
        pltpu.VMEM((6, 8, 512), F32),
        pltpu.VMEM((8, 512), F32),
        pltpu.VMEM((144, 128), F32),
        pltpu.VMEM((128, 128), F32),
        pltpu.VMEM((32, 768), BF),
        pltpu.SemaphoreType.DMA((12,)),
        pltpu.SemaphoreType.DMA((20,)),
        pltpu.SemaphoreType.DMA((20,)),
    ]
    out = pl.pallas_call(
        kernel,
        out_shape=jax.ShapeDtypeStruct((32, NZT), F32),
        in_specs=[any_spec] * 3 + [vmem_spec, smem_spec, vmem_spec] + [any_spec] * 3 + [vmem_spec] * 2,
        out_specs=vmem_spec,
        scratch_shapes=scratch,
        compiler_params=pltpu.CompilerParams(
            collective_id=0, has_side_effects=True, vmem_limit_bytes=64000000
        ),
        name="fno_grad",
    )(
        cotangent.reshape(C, 4, 8, NZT),
        pre_activations.reshape(2, C, 4, 8, NZT),
        spectral_weights.transpose(0, 2, 3, 4, 1, 5),
        skip_weights.transpose(1, 0, 2),
        lift_weights,
        lift_weights.reshape(1, C),
        bf(plane_table()),
        bf(forward_x_table),
        bf(back_x_table),
        bf(y_table()),
        bf(y_back_table()),
    )
    return out.reshape(1, 4, 8, NZT)


def solution(mesh):
    return jax.shard_map(
        per_device,
        mesh=mesh,
        in_specs=(
            P(None, None, "aa", "ba", None),
            P(None, None, None, "aa", "ba", None),
            P(None, None, None, None, "ba", "aa"),
            P(),
            P(),
        ),
        out_specs=P(None, "aa", "ba", None),
        check_vma=False,
    )
```

```python
import math

import jax
import jax.numpy as jnp
import numpy as np
from jax import lax
from jax.experimental import pallas as pl
from jax.experimental.pallas import tpu as pltpu
from jax.sharding import PartitionSpec as P

C = 20
NZT = 2048
NA = 16
NB = 8
NG = 4
START = (0, 3, 10, 17)
COUNT = (3, 7, 7, 3)
WIDTH = (128, 256, 256, 128)
LM = 36
SCALE_ZT = 1.0 / NZT
BF = jnp.bfloat16
F32 = jnp.float32
INV_SQRT2 = 1.0 / math.sqrt(2.0)
INV_SQRT2PI = 1.0 / math.sqrt(2.0 * math.pi)


def freq(count):
    j = np.arange(count)
    return np.where(j < count // 2, j, j - count)


def plane_table():
    joint = np.arange(24 * 12)
    kz = freq(24)[joint // 12]
    kt = joint % 12
    cell = np.arange(NZT)
    turns = (kz[None, :] * (cell[:, None] // 32) * 32 + kt[None, :] * (cell[:, None] % 32) * 64) % NZT
    angle = 2.0 * np.pi / NZT * turns
    table = np.zeros((NZT, 768))
    owner, local = joint // 18, joint % 18
    column = 128 * (owner // 3) + LM * (owner % 3) + 2 * local
    table[:, column] = np.cos(angle)
    table[:, column + 1] = -np.sin(angle)
    return table


def line_angle():
    return 2.0 * np.pi / 64 * ((freq(24)[:, None] * np.arange(64)[None, :]) % 64)


def x_table():
    angle = line_angle()
    out = np.zeros((2, NB, 4, 8, 64, 8))
    for y in range(8):
        out[0, :, :3, y, :, y] = np.cos(angle).reshape(NB, 3, 64)
        out[1, :, :3, y, :, y] = np.sin(angle).reshape(NB, 3, 64)
    return out.reshape(2, 256, 512)


def y_table():
    angle = line_angle().reshape(24, NB, 8)
    out = np.zeros((2, 80, NB, 4, 8))
    for k in range(3):
        out[0, 24 * k : 24 * k + 24, :, k] = np.cos(angle)
        out[1, 24 * k : 24 * k + 24, :, k] = np.sin(angle)
    return out.reshape(2, 80, 256)


def y_back_table():
    wide = np.zeros((2, 256, 128))
    wide[:, :, :80] = y_table().transpose(0, 2, 1) / 64
    return wide


def quarter_signs():
    joint = np.arange(24 * 12)
    rest = freq(24)[joint // 12] % 4
    owner, local = joint // 18, joint % 18
    column = 128 * (owner // 3) + LM * (owner % 3) + 2 * local
    table = np.zeros((8, 768))
    for part in range(2):
        table[0, column + part] = rest % 2 == 0
        table[1, column + part] = np.where(rest % 2 == 0, 1 - rest, 0)
        table[2, column + part] = rest % 2
        table[3, column + part] = np.where(rest % 2 == 1, rest - 2, 0)
    return table


def swap(values):
    even = lax.broadcasted_iota(jnp.int32, (values.shape[0], 128), 1) % 2 == 0
    parts = []
    for t in range(values.shape[1] // 128):
        part = values[:, 128 * t : 128 * t + 128]
        parts.append(jnp.where(even, pltpu.roll(part, 127, 1), -pltpu.roll(part, 1, 1)))
    return parts[0] if len(parts) == 1 else jnp.concatenate(parts, 1)


def dot(a, b):
    return jnp.dot(a, b, preferred_element_type=F32)


def dot_nt(a, b):
    return lax.dot_general(a, b, (((1,), (1,)), ((), ())), preferred_element_type=F32)


def slope_of(v):
    normal_cdf = 0.5 + 0.5 * lax.erf(v * INV_SQRT2)
    return normal_cdf + v * (jnp.exp(-0.5 * v * v) * INV_SQRT2PI)


def loop(count, body):
    lax.fori_loop(0, count, lambda i, carry: (body(i), carry)[1], 0)


def kernel(
    cot_h, pre_h, wts_h, skip_h, lift_h, plane_h, xf_h, xb_h, yf_h, yb_h, signs_h, out_ref,
    cot, pre, wts, skip_ref, lift_ref, plane, xf, xb, yf_ref, yb_ref, signs,
    g1, g0, slope0, skip1, bx, kron, wide,
    s1n, r1n, s2n, r2n, s3n, r3n, s4n, r4n, t1n, q1n, t2n, q2n,
    s1w, r1w, s2w, r2w, s3w, r3w, s4w, r4w, t1w, q1w, t2w, q2w,
    t3, q3, t4, q4,
    q, sm, mm, mg, mt, weff, fold, fa, vv, mt0, bx0, lift_rows,
    in_sem, send_sem, recv_sem,
):
    me_a = lax.axis_index("aa")
    me_b = lax.axis_index("ba")
    lane = lax.broadcasted_iota(jnp.int32, (8, 128), 1)
    row8 = lax.broadcasted_iota(jnp.int32, (8, 128), 0)

    def lanes(rows):
        return lax.broadcasted_iota(jnp.int32, (rows, 128), 1)

    def boxes(narrow, wide_box):
        return [narrow.at[0], wide_box.at[0], wide_box.at[1], narrow.at[1]]

    s1, r1, s2, r2 = boxes(s1n, s1w), boxes(r1n, r1w), boxes(s2n, s2w), boxes(r2n, r2w)
    s3, r3, s4, r4 = boxes(s3n, s3w), boxes(r3n, r3w), boxes(s4n, s4w), boxes(r4n, r4w)
    t1, q1, t2, q2 = boxes(t1n, t1w), boxes(q1n, q1w), boxes(t2n, t2w), boxes(q2n, q2w)

    loads = []
    for g in range(NG):
        part = pl.ds(START[g], COUNT[g])
        loads.append(pltpu.make_async_copy(cot_h.at[part], cot.at[part], in_sem.at[2 * g]))
        loads.append(pltpu.make_async_copy(pre_h.at[1, part], pre.at[1, part], in_sem.at[2 * g + 1]))
    load_plane = pltpu.make_async_copy(plane_h, plane, in_sem.at[8])
    load_pre0 = pltpu.make_async_copy(pre_h.at[0], pre.at[0], in_sem.at[9])
    load_xf = pltpu.make_async_copy(xf_h, xf, in_sem.at[10])
    load_xb = pltpu.make_async_copy(xb_h, xb, in_sem.at[11])
    load_w1 = pltpu.make_async_copy(wts_h.at[1], wts.at[1], in_sem.at[12])
    load_w0 = pltpu.make_async_copy(wts_h.at[0], wts.at[0], in_sem.at[13])
    load_yf = pltpu.make_async_copy(yf_h, yf_ref, in_sem.at[14])
    load_yb = pltpu.make_async_copy(yb_h, yb_ref, in_sem.at[15])
    load_skip = pltpu.make_async_copy(skip_h, skip_ref, in_sem.at[16])
    load_lift = pltpu.make_async_copy(lift_h, lift_ref, in_sem.at[17])
    load_signs = pltpu.make_async_copy(signs_h, signs, in_sem.at[18])
    loads[0].start()
    loads[1].start()
    load_plane.start()

    barrier = pltpu.get_barrier_semaphore()

    def greet_a(d):
        peer = lax.rem(me_a + d + 1, NA)
        pl.semaphore_signal(barrier, 1, device_id={"aa": peer}, device_id_type=pl.DeviceIdType.MESH)

    def greet_b(d):
        peer = lax.rem(me_b + d + 1, NB)
        pl.semaphore_signal(barrier, 1, device_id={"ba": peer}, device_id_type=pl.DeviceIdType.MESH)

    loop(NA - 1, greet_a)
    loop(NB - 1, greet_b)

    for box in (r2n, r3n, q2n, r2w, r3w, q2w, q3):
        box[..., 24:32, :] = jnp.zeros(box.shape[:-2] + (8, box.shape[-1]), BF)
    mm[...] = jnp.zeros(mm.shape, F32)
    mt[...] = jnp.zeros(mt.shape, F32)
    mt0[...] = jnp.zeros(mt0.shape, F32)
    weff[...] = jnp.zeros(weff.shape, F32)
    fold[...] = jnp.zeros(fold.shape, F32)
    sm[...] = jnp.zeros(sm.shape, F32)

    def partners(axis):
        if axis == "aa":
            order = [
                (1, 2, 0), (1, 2, 1), (1, 1, 0), (1, 3, 0), (1, 1, 1), (1, 3, 1), (1, 0, 0), (1, 0, 1),
                (0, 2, 0), (0, 2, 1), (0, 1, 0), (0, 3, 0), (0, 1, 1), (0, 3, 1), (0, 0, 1),
            ]
            z, x, core = me_a // 8, lax.rem(me_a // 2, 4), lax.rem(me_a, 2)
            return [
                lax.rem(z + dz, 2) * 8 + lax.rem(x + dx, 4) * 2 + lax.rem(core + dc, 2)
                for dz, dx, dc in order
            ]
        z, y = me_b // 4, lax.rem(me_b, 4)
        order = [(1, 2), (0, 2), (1, 1), (1, 3), (0, 1), (0, 3), (1, 0)]
        return [lax.rem(z + dz, 2) * 4 + lax.rem(y + dy, 4) for dz, dy in order]

    def send(axis, src, dst, slot):
        me = me_a if axis == "aa" else me_b
        rows = pl.ds(0, 32 if axis == "aa" else 24)
        for peer in partners(axis):
            pltpu.make_async_remote_copy(
                src_ref=src.at[peer, rows],
                dst_ref=dst.at[me, rows],
                send_sem=send_sem.at[slot],
                recv_sem=recv_sem.at[slot],
                device_id={axis: peer},
                device_id_type=pl.DeviceIdType.MESH,
            ).start()
        dst[me] = src[me]

    def span(axis, box):
        if axis == "aa":
            return box.at[pl.ds(0, NA - 1)]
        return box.at[pl.ds(0, NB - 1), pl.ds(0, 24)]

    def arrive(axis, dst, slot):
        part = span(axis, dst)
        pltpu.make_async_copy(part, part, recv_sem.at[slot]).wait()

    def drain(axis, src, slot):
        part = span(axis, src)
        pltpu.make_async_copy(part, part, send_sem.at[slot]).wait()

    def forward_zt(field, g, dst):
        values = field[START[g] : START[g] + COUNT[g]].reshape(COUNT[g] * 32, NZT)
        for block in range(3):
            out = dot(values, plane[:, 256 * block : 256 * block + 256])
            for a in range(6 * block, min(6 * block + 6, NA)):
                t, j = a // 3 - 2 * block, a % 3
                low = high = None
                for c in range(COUNT[g]):
                    piece = out[32 * c : 32 * c + 32, 128 * t : 128 * t + 128]
                    shift = (LM * c - LM * j) % 128
                    if shift:
                        piece = pltpu.roll(piece, shift, 1)
                    start = LM * c
                    if start < 128:
                        low = piece if low is None else jnp.where(lanes(32) < start, low, piece)
                    if start + LM > 128:
                        high = piece if high is None else jnp.where(lanes(32) < start - 128, high, piece)
                dst[a, :, 0:128] = low.astype(BF)
                if high is not None:
                    dst[a, :, 128:256] = high.astype(BF)

    def forward_x(src, dst, g):
        values = src[...].reshape(512, WIDTH[g])
        out = dot(xf[0], values) + swap(dot(xf[1], values))
        dst[...] = out.astype(BF).reshape(NB, 32, WIDTH[g])

    def forward_y(src, g):
        size = WIDTH[g]
        values = src[...].reshape(256, size)
        out = dot(yf_ref[0], values) + swap(dot(yf_ref[1], values))
        full = jnp.concatenate([out, jnp.zeros((48, size), F32)], 0)
        q[0:size] = full.T
        for p in range(2):
            tiles = [[None] * 4 for _ in range(3)]
            for m in range(18):
                rows = q[pl.ds(2 * m + p, 8, stride=LM), :]
                rows = jnp.where(row8 < COUNT[g], rows, 0.0)
                t, off = divmod(24 * m, 128)
                for k in range(3):
                    shift = (24 * m - 24 * k) % 128
                    piece = pltpu.roll(rows, shift, 1) if shift else rows
                    old = tiles[k][t]
                    tiles[k][t] = piece if old is None else jnp.where(lane < off, old, piece)
                    if off + 24 > 128:
                        tiles[k][t + 1] = piece
            for k in range(3):
                for t in range(4):
                    sm[k, p, g, :, 128 * t : 128 * t + 128] = tiles[k][t]

    def mix(g):
        def one(k):
            for t in range(4):
                size = 128 if t < 3 else 48
                part = slice(128 * t, 128 * t + size)
                by_re = mm[k, 0, t, 0:40, 0:size]
                by_im = mm[k, 1, t, 0:40, 0:size]
                all_re = sm[k, 0, g, :, part]
                all_im = sm[k, 1, g, :, part]
                for c in range(COUNT[g]):
                    w = wide[START[g] + c, k, :, part]
                    by_re = by_re + w * all_re[c : c + 1]
                    by_im = by_im + w * all_im[c : c + 1]
                mm[k, 0, t, 0:40, 0:size] = by_re
                mm[k, 1, t, 0:40, 0:size] = by_im

        loop(3, one)

    def unmix(g):
        first, second = pl.ds(2 * START[g], 8, stride=2), pl.ds(2 * START[g] + 1, 8, stride=2)
        for k in range(3):
            for t in range(4):
                part = slice(128 * t, 128 * t + 128)
                mg[k, 0, :, part] = mm[k, 0, t, first, :] + mm[k, 1, t, second, :]
                mg[k, 1, :, part] = mm[k, 1, t, first, :] - mm[k, 0, t, second, :]

    def tile_of(load, m):
        t, off = divmod(24 * m, 128)
        value = load(t)
        if off + 24 > 128:
            value = jnp.where(lane < 64, load(t + 1), value)
        return value

    def back_y(dst, g):
        for m in range(18):
            for p in range(2):
                parts = []
                for k in range(3):
                    value = tile_of(lambda t: mg[k, p, :, 128 * t : 128 * t + 128], m)
                    shift = (24 * k - 24 * m) % 128
                    parts.append(pltpu.roll(value, shift, 1) if shift else value)
                row = jnp.where(lane < 24, parts[0], jnp.where(lane < 48, parts[1], parts[2]))
                mt[pl.ds(2 * m + p, 8, stride=LM), :] = row
        values = mt[0 : WIDTH[g]].astype(BF)
        out = dot_nt(yb_ref[0], values) - swap(dot_nt(yb_ref[1], values))
        dst[...] = out.astype(BF).reshape(NB, 32, WIDTH[g])

    def back_x(values):
        turned = -swap(values.astype(F32))
        return dot(xb[0], values) + dot(xb[1], turned.astype(BF))

    def unpack(src, g):
        for c in range(COUNT[g]):
            start = LM * c
            low = start // 128
            for t in range(6):
                full = None
                for j in range(3 if t < 5 else 1):
                    a = 3 * t + j
                    value = src[a, :, 128 * low : 128 * low + 128].astype(F32)
                    if start % 128 + LM > 128:
                        value = jnp.where(lanes(32) < 64, src[a, :, 128:256].astype(F32), value)
                    shift = (LM * j - start) % 128
                    value = pltpu.roll(value, shift, 1) if shift else value
                    full = value if full is None else jnp.where(lanes(32) < LM * j, full, value)
                bx[32 * c : 32 * c + 32, 128 * t : 128 * t + 128] = full.astype(BF)

    def grad_top(g):
        def one(i):
            c = START[g] + i
            for pair in range(2):
                for n in range(4):
                    part = slice(512 * n, 512 * n + 512)
                    v = pre[1, c, 2 * pair : 2 * pair + 2, :, part].astype(F32).reshape(16, 512)
                    d = cot[c, 2 * pair : 2 * pair + 2, :, part].astype(F32).reshape(16, 512)
                    g1[c, 16 * pair : 16 * pair + 16, part] = (d * slope_of(v)).astype(BF)

        loop(COUNT[g], one)

    for g in range(NG):
        loads[2 * g].wait()
        loads[2 * g + 1].wait()
        if g == 0:
            for copy in loads[2:4]:
                copy.start()
        grad_top(g)
        if g == 0:
            load_plane.wait()
            late = [load_skip, load_w1, load_xf, load_yf, load_yb, load_xb, load_lift, load_w0, load_pre0, load_signs]
            for copy in loads[4:] + late:
                copy.start()
        forward_zt(g1, g, s1[g])
        if g == 0:
            pl.semaphore_wait(barrier, NA + NB - 2)
        send("aa", s1[g], r1[g], g)

    def spread(rows, groups):
        r = lax.broadcasted_iota(jnp.int32, (rows, groups), 0) // 16
        return (r == lax.broadcasted_iota(jnp.int32, (rows, groups), 1)).astype(BF)

    load_skip.wait()
    skip_all = skip_ref[...].astype(F32)
    left = dot_nt(spread(320, C), skip_all[:, 1, :].astype(BF)).astype(BF)
    whole = dot_nt(left, spread(320, C))
    same = lax.broadcasted_iota(jnp.int32, (320, 320), 0) % 16 == lax.broadcasted_iota(jnp.int32, (320, 320), 1) % 16
    kron[...] = jnp.where(same, whole, 0.0).astype(BF)
    load_w1.wait()

    def widen(o):
        for k in range(3):
            for t in range(4):
                part = slice(128 * t, min(128 * t + 128, 432))
                wide[o, k, :, part] = wts[1, o, :, k, :, part].reshape(40, part.stop - part.start).astype(F32)

    loop(C, widen)
    load_xf.wait()

    def stage_x1(g):
        arrive("aa", r1[g], g)
        forward_x(r1[g], s2[g], g)
        send("ba", s2[g], r2[g], 4 + g)

    stage_x1(0)

    def skip_piece1(n):
        part = pl.ds(pl.multiple_of(512 * n, 512), 512)
        for pair in range(2):
            rows = slice(16 * pair, 16 * pair + 16)
            out = dot(kron[...], g1[:, rows, part].reshape(320, 512))
            skip1[:, rows, part] = out.reshape(C, 16, 512)

    loop(4, skip_piece1)
    for g in range(1, NG):
        stage_x1(g)

    load_yf.wait()
    for g in range(NG):
        arrive("ba", r2[g], 4 + g)
        forward_y(r2[g], g)
        mix(g)

    load_yb.wait()
    for g in range(NG):
        unmix(g)
        back_y(s3[g], g)
        send("ba", s3[g], r3[g], 8 + g)

    load_lift.wait()
    for i in range(C):
        lift_rows[i] = jnp.broadcast_to(lift_ref[:, i : i + 1], (2, 128))
    load_w0.wait()

    def fold_weights(k):
        for t in range(4):
            part = slice(128 * t, min(128 * t + 128, 432))
            size = part.stop - part.start
            for o in range(C):
                total = wts[0, o, 0, k, :, part].astype(F32) * lift_rows[0, :, 0:size]
                for i in range(1, C):
                    total = total + wts[0, o, i, k, :, part].astype(F32) * lift_rows[i, :, 0:size]
                weff[k, 0, o : o + 1, part] = total[0:1]
                weff[k, 1, o : o + 1, part] = total[1:2]

    loop(3, fold_weights)
    load_xb.wait()
    for g in range(NG):
        arrive("ba", r3[g], 8 + g)
        out = back_x(r3[g][...].reshape(256, WIDTH[g]))
        s4[g][...] = out.astype(BF).reshape(NA, 32, WIDTH[g])
        send("aa", s4[g], r4[g], 12 + g)

    load_pre0.wait()

    def slope_one(c):
        for pair in range(2):
            for n in range(4):
                part = slice(512 * n, 512 * n + 512)
                v = pre[0, c, 2 * pair : 2 * pair + 2, :, part].astype(F32).reshape(16, 512)
                slope0[c, 16 * pair : 16 * pair + 16, part] = slope_of(v)

    loop(C, slope_one)

    for g in range(NG):
        arrive("aa", r4[g], 12 + g)
        unpack(r4[g], g)

        def piece(n):
            part = pl.ds(pl.multiple_of(512 * n, 512), 512)
            spectral = dot_nt(bx[0 : 32 * COUNT[g]], plane[part, :]).reshape(COUNT[g], 32, 512)
            for c in range(COUNT[g]):
                o = START[g] + c
                incoming = skip1[o, :, part] + spectral[c] * SCALE_ZT
                g0[o, :, part] = (incoming * slope0[o, :, part]).astype(BF)

        loop(4, piece)
        forward_zt(g0, g, t1[g])
        send("aa", t1[g], q1[g], 16 + g)

    for g in range(NG):
        arrive("aa", q1[g], 16 + g)
        forward_x(q1[g], t2[g], g)
        send("ba", t2[g], q2[g], 20 + g)

    gain = jnp.sum(skip_all[:, 0, :] * lift_ref[...], 1, keepdims=True)

    def skip_piece(n):
        part = pl.ds(pl.multiple_of(512 * n, 512), 512)
        for pair in range(2):
            rows = slice(16 * pair, 16 * pair + 16)
            total = jnp.zeros((16, 512), F32)
            for c in range(C):
                total = total + g0[c, rows, part].astype(F32) * gain[c : c + 1, :]
            out_ref[rows, part] = total

    loop(4, skip_piece)

    for g in range(NG):
        arrive("ba", q2[g], 20 + g)
        forward_y(q2[g], g)
        rows = slice(START[g], START[g] + 8)
        for k in range(3):
            w_re, w_im = weff[k, 0, rows, :], weff[k, 1, rows, :]
            s_re, s_im = sm[k, 0, g], sm[k, 1, g]
            fold[k] += w_re * s_re + w_im * s_im
            fold[3 + k] += w_re * s_im - w_im * s_re

    for i in range(6):
        fa[i : i + 1] = jnp.sum(fold[i], 0, keepdims=True)
    fa[6:8] = jnp.zeros((2, 512), F32)
    for m in range(18):
        value = tile_of(lambda t: fa[:, 128 * t : 128 * t + 128], m)
        shift = (-24 * m) % 128
        vv[8 * m : 8 * m + 8] = pltpu.roll(value, shift, 1) if shift else value
    for p in range(2):
        parts = []
        for k in range(3):
            value = vv[pl.ds(3 * p + k, 18, stride=8), :]
            parts.append(pltpu.roll(value, 24 * k, 1) if k else value)
        full = jnp.where(lanes(18) < 24, parts[0], jnp.where(lanes(18) < 48, parts[1], parts[2]))
        mt0[pl.ds(p, 18, stride=2), :] = full
    values = mt0[...].astype(BF)
    out = dot_nt(yb_ref[0], values) - swap(dot_nt(yb_ref[1], values))
    t3[...] = out.astype(BF).reshape(NB, 32, 128)
    send("ba", t3, q3, 24)
    arrive("ba", q3, 24)
    t4[...] = back_x(q3[...].reshape(256, 128)).astype(BF).reshape(NA, 32, 128)
    send("aa", t4, q4, 25)
    load_signs.wait()
    arrive("aa", q4, 25)
    for t in range(6):
        part = slice(128 * t, 128 * t + 128)
        full = None
        for j in range(3 if t < 5 else 1):
            value = q4[3 * t + j].astype(F32)
            if j:
                value = jnp.where(lanes(32) < LM * j, full, pltpu.roll(value, LM * j, 1))
            full = value
        turned = swap(full)
        for i in range(4):
            variant = (turned if i == 3 else full) * signs[i : i + 1, part]
            bx0[32 * i : 32 * i + 32, part] = variant.astype(BF)
    quarter = dot_nt(bx0[...], plane[0:512, :]) * SCALE_ZT
    even, half, odd, turn = [quarter[32 * i : 32 * i + 32] for i in range(4)]
    out_ref[:, 0:512] += even + odd
    out_ref[:, 512:1024] += half + turn
    out_ref[:, 1024:1536] += even - odd
    out_ref[:, 1536:2048] += half - turn

    for g in range(NG):
        drain("aa", s1[g], g)
        drain("ba", s2[g], 4 + g)
        drain("ba", s3[g], 8 + g)
        drain("aa", s4[g], 12 + g)
        drain("aa", t1[g], 16 + g)
        drain("ba", t2[g], 20 + g)
    drain("ba", t3, 24)
    drain("aa", t4, 25)


def per_device(cotangent, pre_activations, spectral_weights, skip_weights, lift_weights):
    bf = lambda table: jnp.asarray(table.astype(np.float32), dtype=BF)
    forward_x_table = x_table()
    back_x_table = forward_x_table.transpose(0, 2, 1) / 64
    any_spec = pl.BlockSpec(memory_space=pl.ANY)
    kinds = [NA, NA, NB, NB, NB, NB, NA, NA, NA, NA, NB, NB]
    scratch = [
        pltpu.VMEM((C, 4, 8, NZT), BF),
        pltpu.VMEM((2, C, 4, 8, NZT), BF),
        pltpu.VMEM((2, C, C, 3, 2, 432), BF),
        pltpu.VMEM((C, 2, C), BF),
        pltpu.VMEM((1, C), F32),
        pltpu.VMEM((NZT, 768), BF),
        pltpu.VMEM((2, 256, 512), BF),
        pltpu.VMEM((2, 512, 256), BF),
        pltpu.VMEM((2, 80, 256), BF),
        pltpu.VMEM((2, 256, 128), BF),
        pltpu.VMEM((8, 768), F32),
        pltpu.VMEM((C, 32, NZT), BF),
        pltpu.VMEM((C, 32, NZT), BF),
        pltpu.VMEM((C, 32, NZT), F32),
        pltpu.VMEM((C, 32, NZT), F32),
        pltpu.VMEM((224, 768), BF),
        pltpu.VMEM((320, 320), BF),
        pltpu.VMEM((C, 3, 40, 432), F32),
        *[pltpu.VMEM((2, size, 32, 128), BF) for size in kinds],
        *[pltpu.VMEM((2, size, 32, 256), BF) for size in kinds],
        pltpu.VMEM((NB, 32, 128), BF), pltpu.VMEM((NB, 32, 128), BF),
        pltpu.VMEM((NA, 32, 128), BF), pltpu.VMEM((NA, 32, 128), BF),
        pltpu.VMEM((296, 128), F32),
        pltpu.VMEM((3, 2, NG, 8, 512), F32),
        pltpu.VMEM((3, 2, 4, 56, 128), F32),
        pltpu.VMEM((3, 2, 8, 512), F32),
        pltpu.VMEM((296, 128), F32),
        pltpu.VMEM((3, 2, 32, 512), F32),
        pltpu.VMEM((6, 8, 512), F32),
        pltpu.VMEM((8, 512), F32),
        pltpu.VMEM((144, 128), F32),
        pltpu.VMEM((128, 128), F32),
        pltpu.VMEM((128, 768), BF),
        pltpu.VMEM((C, 2, 128), F32),
        pltpu.SemaphoreType.DMA((19,)),
        pltpu.SemaphoreType.DMA((26,)),
        pltpu.SemaphoreType.DMA((26,)),
    ]
    out = pl.pallas_call(
        kernel,
        out_shape=jax.ShapeDtypeStruct((32, NZT), F32),
        in_specs=[any_spec] * 11,
        out_specs=pl.BlockSpec(memory_space=pltpu.VMEM),
        scratch_shapes=scratch,
        compiler_params=pltpu.CompilerParams(
            collective_id=0, has_side_effects=True, vmem_limit_bytes=66000000
        ),
        name="fno_grad",
    )(
        cotangent.reshape(C, 4, 8, NZT),
        pre_activations.reshape(2, C, 4, 8, NZT),
        spectral_weights.transpose(0, 2, 3, 4, 1, 5),
        skip_weights.transpose(1, 0, 2),
        lift_weights.reshape(1, C),
        bf(plane_table()),
        bf(forward_x_table),
        bf(back_x_table),
        bf(y_table()),
        bf(y_back_table()),
        jnp.asarray(quarter_signs(), F32),
    )
    return out.reshape(1, 4, 8, NZT)


def solution(mesh):
    return jax.shard_map(
        per_device,
        mesh=mesh,
        in_specs=(
            P(None, None, "aa", "ba", None),
            P(None, None, None, "aa", "ba", None),
            P(None, None, None, None, "ba", "aa"),
            P(),
            P(),
        ),
        out_specs=P(None, "aa", "ba", None),
        check_vma=False,
    )
```

```python
import math

import jax
import jax.numpy as jnp
import numpy as np
from jax import lax
from jax.experimental import pallas as pl
from jax.experimental.pallas import tpu as pltpu
from jax.sharding import PartitionSpec as P

C = 20
NZT = 2048
NA = 16
NB = 8
NG = 4
START = (0, 3, 10, 17)
COUNT = (3, 7, 7, 3)
WIDTH = (128, 256, 256, 128)
LM = 36
SCALE_ZT = 1.0 / NZT
BF = jnp.bfloat16
F32 = jnp.float32
INV_SQRT2 = 1.0 / math.sqrt(2.0)
INV_SQRT2PI = 1.0 / math.sqrt(2.0 * math.pi)


def freq(count):
    j = np.arange(count)
    return np.where(j < count // 2, j, j - count)


def plane_table():
    cell = np.arange(512)
    kt = np.arange(12)
    table = np.zeros((6, 512, 256))
    for f in range(24):
        kz, rest, place = freq(24)[f], f % 4, f // 4
        column = (24 * place if place < 5 else 128) + 2 * kt
        turns = (kz * (cell[:, None] // 32) * 32 + kt[None, :] * (cell[:, None] % 32) * 64) % NZT
        angle = 2.0 * np.pi / NZT * turns
        index = {0: 0, 2: 1, 1: 2, 3: 3}[rest]
        table[index][:, column] = np.cos(angle)
        table[index][:, column + 1] = -np.sin(angle)
        if rest % 2:
            sign = -1 if rest == 1 else 1
            table[index + 2][:, column] = sign * np.sin(angle)
            table[index + 2][:, column + 1] = sign * np.cos(angle)
    return table


CLASS = (0, 2, 1, 3)


def slot(f):
    return 24 * (f // 4) if f < 20 else 128


def pieces_of(a):
    u = a // 2
    if a % 2 == 0:
        return [(3 * u, 0, 24, 0), (3 * u + 1, 0, 12, 24)]
    return [(3 * u + 1, 12, 12, 0), (3 * u + 2, 0, 24, 12)]


def line_angle():
    return 2.0 * np.pi / 64 * ((freq(24)[:, None] * np.arange(64)[None, :]) % 64)


def x_table():
    angle = line_angle()
    out = np.zeros((2, NB, 4, 8, 64, 8))
    for y in range(8):
        out[0, :, :3, y, :, y] = np.cos(angle).reshape(NB, 3, 64)
        out[1, :, :3, y, :, y] = np.sin(angle).reshape(NB, 3, 64)
    return out.reshape(2, 256, 512)


def y_table():
    angle = line_angle().reshape(24, NB, 8)
    out = np.zeros((2, 80, NB, 4, 8))
    for k in range(3):
        out[0, 24 * k : 24 * k + 24, :, k] = np.cos(angle)
        out[1, 24 * k : 24 * k + 24, :, k] = np.sin(angle)
    return out.reshape(2, 80, 256)


def y_back_table():
    wide = np.zeros((2, 256, 128))
    wide[:, :, :80] = y_table().transpose(0, 2, 1) / 64
    return wide


def swap(values):
    even = lax.broadcasted_iota(jnp.int32, (values.shape[0], 128), 1) % 2 == 0
    parts = []
    for t in range(values.shape[1] // 128):
        part = values[:, 128 * t : 128 * t + 128]
        parts.append(jnp.where(even, pltpu.roll(part, 127, 1), -pltpu.roll(part, 1, 1)))
    return parts[0] if len(parts) == 1 else jnp.concatenate(parts, 1)


def dot(a, b):
    return jnp.dot(a, b, preferred_element_type=F32)


def dot_nt(a, b):
    return lax.dot_general(a, b, (((1,), (1,)), ((), ())), preferred_element_type=F32)


def slope_of(v):
    normal_cdf = 0.5 + 0.5 * lax.erf(v * INV_SQRT2)
    return normal_cdf + v * (jnp.exp(-0.5 * v * v) * INV_SQRT2PI)


def loop(count, body):
    lax.fori_loop(0, count, lambda i, carry: (body(i), carry)[1], 0)


def kernel(
    cot_h, pre_h, wts_h, skip_h, lift_h, plane_h, xf_h, xb_h, yf_h, yb_h, out_ref,
    cot, pre, wts, skip_ref, lift_ref, plane, xf, xb, yf_ref, yb_ref,
    g1, g0, slope0, skip1, bx, pz, kron, wide,
    s1n, r1n, s2n, r2n, s3n, r3n, s4n, r4n, t1n, q1n, t2n, q2n,
    s1w, r1w, s2w, r2w, s3w, r3w, s4w, r4w, t1w, q1w, t2w, q2w,
    t3, q3, t4, q4,
    q, sm, mm, mg, mt, weff, fold, lifted, lift_rows,
    in_sem, send_sem, recv_sem,
):
    me_a = lax.axis_index("aa")
    me_b = lax.axis_index("ba")
    lane = lax.broadcasted_iota(jnp.int32, (8, 128), 1)
    row8 = lax.broadcasted_iota(jnp.int32, (8, 128), 0)

    def lanes(rows):
        return lax.broadcasted_iota(jnp.int32, (rows, 128), 1)

    def boxes(narrow, wide_box):
        return [narrow.at[0], wide_box.at[0], wide_box.at[1], narrow.at[1]]

    s1, r1, s2, r2 = boxes(s1n, s1w), boxes(r1n, r1w), boxes(s2n, s2w), boxes(r2n, r2w)
    s3, r3, s4, r4 = boxes(s3n, s3w), boxes(r3n, r3w), boxes(s4n, s4w), boxes(r4n, r4w)
    t1, q1, t2, q2 = boxes(t1n, t1w), boxes(q1n, q1w), boxes(t2n, t2w), boxes(q2n, q2w)

    loads = []
    for g in range(NG):
        part = pl.ds(START[g], COUNT[g])
        loads.append(pltpu.make_async_copy(cot_h.at[part], cot.at[part], in_sem.at[2 * g]))
        loads.append(pltpu.make_async_copy(pre_h.at[1, part], pre.at[1, part], in_sem.at[2 * g + 1]))
    load_plane = pltpu.make_async_copy(plane_h, plane, in_sem.at[8])
    load_pre0 = pltpu.make_async_copy(pre_h.at[0], pre.at[0], in_sem.at[9])
    load_xf = pltpu.make_async_copy(xf_h, xf, in_sem.at[10])
    load_xb = pltpu.make_async_copy(xb_h, xb, in_sem.at[11])
    load_w1 = pltpu.make_async_copy(wts_h.at[1], wts.at[1], in_sem.at[12])
    load_w0 = pltpu.make_async_copy(wts_h.at[0], wts.at[0], in_sem.at[13])
    load_yf = pltpu.make_async_copy(yf_h, yf_ref, in_sem.at[14])
    load_yb = pltpu.make_async_copy(yb_h, yb_ref, in_sem.at[15])
    load_skip = pltpu.make_async_copy(skip_h, skip_ref, in_sem.at[16])
    load_lift = pltpu.make_async_copy(lift_h, lift_ref, in_sem.at[17])
    loads[0].start()
    loads[1].start()
    load_plane.start()

    barrier = pltpu.get_barrier_semaphore()

    def greet_a(d):
        peer = lax.rem(me_a + d + 1, NA)
        pl.semaphore_signal(barrier, 1, device_id={"aa": peer}, device_id_type=pl.DeviceIdType.MESH)

    def greet_b(d):
        peer = lax.rem(me_b + d + 1, NB)
        pl.semaphore_signal(barrier, 1, device_id={"ba": peer}, device_id_type=pl.DeviceIdType.MESH)

    loop(NA - 1, greet_a)
    loop(NB - 1, greet_b)

    for box in (r2n, r3n, q2n, r2w, r3w, q2w, q3):
        box[..., 24:32, :] = jnp.zeros(box.shape[:-2] + (8, box.shape[-1]), BF)
    mm[...] = jnp.zeros(mm.shape, F32)
    mt[...] = jnp.zeros(mt.shape, F32)
    weff[...] = jnp.zeros(weff.shape, F32)
    fold[...] = jnp.zeros(fold.shape, F32)
    sm[...] = jnp.zeros(sm.shape, F32)

    def partners(axis):
        if axis == "aa":
            order = [
                (1, 2, 0), (1, 2, 1), (1, 1, 0), (1, 3, 0), (1, 1, 1), (1, 3, 1), (1, 0, 0), (1, 0, 1),
                (0, 2, 0), (0, 2, 1), (0, 1, 0), (0, 3, 0), (0, 1, 1), (0, 3, 1), (0, 0, 1),
            ]
            z, x, core = me_a // 8, lax.rem(me_a // 2, 4), lax.rem(me_a, 2)
            return [
                lax.rem(z + dz, 2) * 8 + lax.rem(x + dx, 4) * 2 + lax.rem(core + dc, 2)
                for dz, dx, dc in order
            ]
        z, y = me_b // 4, lax.rem(me_b, 4)
        order = [(1, 2), (0, 2), (1, 1), (1, 3), (0, 1), (0, 3), (1, 0)]
        return [lax.rem(z + dz, 2) * 4 + lax.rem(y + dy, 4) for dz, dy in order]

    def send(axis, src, dst, slot):
        me = me_a if axis == "aa" else me_b
        rows = pl.ds(0, 32 if axis == "aa" else 24)
        for peer in partners(axis):
            pltpu.make_async_remote_copy(
                src_ref=src.at[peer, rows],
                dst_ref=dst.at[me, rows],
                send_sem=send_sem.at[slot],
                recv_sem=recv_sem.at[slot],
                device_id={axis: peer},
                device_id_type=pl.DeviceIdType.MESH,
            ).start()
        dst[me] = src[me]

    def span(axis, box):
        if axis == "aa":
            return box.at[pl.ds(0, NA - 1)]
        return box.at[pl.ds(0, NB - 1), pl.ds(0, 24)]

    def arrive(axis, dst, slot):
        part = span(axis, dst)
        pltpu.make_async_copy(part, part, recv_sem.at[slot]).wait()

    def drain(axis, src, slot):
        part = span(axis, src)
        pltpu.make_async_copy(part, part, send_sem.at[slot]).wait()

    def combine(fields, rows, part):
        sum02, sum13 = fields[0] + fields[2], fields[1] + fields[3]
        pz[0, rows, part] = (sum02 + sum13).astype(BF)
        pz[1, rows, part] = (sum02 - sum13).astype(BF)
        pz[2, rows, part] = (fields[0] - fields[2]).astype(BF)
        pz[3, rows, part] = (fields[1] - fields[3]).astype(BF)

    def forward_zt(g, dst):
        rows = slice(0, 32 * COUNT[g])
        odd, turned = pz[2, rows], pz[3, rows]
        out = [
            dot(pz[0, rows], plane[0]),
            dot(pz[1, rows], plane[1]),
            dot(odd, plane[2]) + dot(turned, plane[4]),
            dot(odd, plane[3]) + dot(turned, plane[5]),
        ]
        for a in range(NA):
            low = high = None
            for c in range(COUNT[g]):
                for f, first, size, place in pieces_of(a):
                    t, source = divmod(slot(f) + first, 128)
                    start = LM * c + place
                    piece = out[CLASS.index(f % 4)][32 * c : 32 * c + 32, 128 * t : 128 * t + 128]
                    shift = (start - source) % 128
                    if shift:
                        piece = pltpu.roll(piece, shift, 1)
                    if start < 128:
                        low = piece if low is None else jnp.where(lanes(32) < start, low, piece)
                    if start + size > 128:
                        high = piece if high is None else jnp.where(lanes(32) < start - 128, high, piece)
            dst[a, :, 0:128] = low.astype(BF)
            if high is not None:
                dst[a, :, 128:256] = high.astype(BF)

    def forward_x(src, dst, g):
        values = src[...].reshape(512, WIDTH[g])
        out = dot(xf[0], values) + swap(dot(xf[1], values))
        dst[...] = out.astype(BF).reshape(NB, 32, WIDTH[g])

    def spectrum_y(src, g):
        values = src[...].reshape(256, WIDTH[g])
        return dot(yf_ref[0], values) + swap(dot(yf_ref[1], values))

    def forward_y(src, g):
        size = WIDTH[g]
        out = spectrum_y(src, g)
        full = jnp.concatenate([out, jnp.zeros((48, size), F32)], 0)
        q[0:size] = full.T
        for p in range(2):
            tiles = [[None] * 4 for _ in range(3)]
            for m in range(18):
                rows = q[pl.ds(2 * m + p, 8, stride=LM), :]
                t, off = divmod(24 * m, 128)
                for k in range(3):
                    shift = (24 * m - 24 * k) % 128
                    piece = pltpu.roll(rows, shift, 1) if shift else rows
                    old = tiles[k][t]
                    tiles[k][t] = piece if old is None else jnp.where(lane < off, old, piece)
                    if off + 24 > 128:
                        tiles[k][t + 1] = piece
            for k in range(3):
                for t in range(4):
                    sm[k, p, g, :, 128 * t : 128 * t + 128] = tiles[k][t]

    def mix(g):
        def one(k):
            for t in range(4):
                size = 128 if t < 3 else 48
                part = slice(128 * t, 128 * t + size)
                by_re = mm[k, 0, t, 0:40, 0:size]
                by_im = mm[k, 1, t, 0:40, 0:size]
                all_re = sm[k, 0, g, :, part]
                all_im = sm[k, 1, g, :, part]
                for c in range(COUNT[g]):
                    w = wide[START[g] + c, k, :, part]
                    by_re = by_re + w * all_re[c : c + 1]
                    by_im = by_im + w * all_im[c : c + 1]
                mm[k, 0, t, 0:40, 0:size] = by_re
                mm[k, 1, t, 0:40, 0:size] = by_im

        loop(3, one)

    def unmix(g):
        first, second = pl.ds(2 * START[g], 8, stride=2), pl.ds(2 * START[g] + 1, 8, stride=2)
        for k in range(3):
            for t in range(4):
                part = slice(128 * t, 128 * t + 128)
                mg[k, 0, :, part] = mm[k, 0, t, first, :] + mm[k, 1, t, second, :]
                mg[k, 1, :, part] = mm[k, 1, t, first, :] - mm[k, 0, t, second, :]

    def tile_of(load, m):
        t, off = divmod(24 * m, 128)
        value = load(t)
        if off + 24 > 128:
            value = jnp.where(lane < 64, load(t + 1), value)
        return value

    def back_y(dst, g):
        for m in range(18):
            for p in range(2):
                parts = []
                for k in range(3):
                    value = tile_of(lambda t: mg[k, p, :, 128 * t : 128 * t + 128], m)
                    shift = (24 * k - 24 * m) % 128
                    parts.append(pltpu.roll(value, shift, 1) if shift else value)
                row = jnp.where(lane < 24, parts[0], jnp.where(lane < 48, parts[1], parts[2]))
                mt[pl.ds(2 * m + p, 8, stride=LM), :] = row
        values = mt[0 : WIDTH[g]].astype(BF)
        out = dot_nt(yb_ref[0], values) - swap(dot_nt(yb_ref[1], values))
        dst[...] = out.astype(BF).reshape(NB, 32, WIDTH[g])

    def back_x(values):
        turned = -swap(values.astype(F32))
        return dot(xb[0], values) + dot(xb[1], turned.astype(BF))

    def unpack(src, count):
        for c in range(count):
            for r in range(4):
                for t in range(2):
                    full = None
                    for f in [r, 4 + r, 8 + r, 12 + r, 16 + r] if t == 0 else [20 + r]:
                        for a in (f // 3 * 2, f // 3 * 2 + 1):
                            for kz, first, size, place in pieces_of(a):
                                if kz != f:
                                    continue
                                low, source = divmod(LM * c + place, 128)
                                value = src[a, :, 128 * low : 128 * low + 128].astype(F32)
                                if source + size > 128:
                                    value = jnp.where(lanes(32) < 64, src[a, :, 128:256].astype(F32), value)
                                start = (slot(f) + first) % 128
                                shift = (start - source) % 128
                                value = pltpu.roll(value, shift, 1) if shift else value
                                full = value if full is None else jnp.where(lanes(32) < start, full, value)
                    bx[CLASS.index(r), 32 * c : 32 * c + 32, 128 * t : 128 * t + 128] = full.astype(BF)

    def inverse_zt(count, h):
        rows, part = slice(0, 32 * count), slice(256 * h, 256 * h + 256)
        even = dot_nt(bx[0, rows], plane[0, part])
        half = dot_nt(bx[1, rows], plane[1, part])
        odd = dot_nt(bx[2, rows], plane[2, part]) + dot_nt(bx[3, rows], plane[3, part])
        turn = dot_nt(bx[2, rows], plane[4, part]) + dot_nt(bx[3, rows], plane[5, part])
        total, rest = even + half, even - half
        return [total + odd, rest + turn, total - odd, rest - turn]

    def grad_top(g):
        def one(i):
            c = START[g] + i
            for pair in range(2):
                for h in range(4):
                    fields = []
                    for n in range(4):
                        part = slice(512 * n + 128 * h, 512 * n + 128 * h + 128)
                        v = pre[1, c, 2 * pair : 2 * pair + 2, :, part].astype(F32).reshape(16, 128)
                        d = cot[c, 2 * pair : 2 * pair + 2, :, part].astype(F32).reshape(16, 128)
                        value = (d * slope_of(v)).astype(BF)
                        g1[c, 16 * pair : 16 * pair + 16, part] = value
                        fields.append(value.astype(F32))
                    rows = pl.ds(pl.multiple_of(32 * i + 16 * pair, 16), 16)
                    combine(fields, rows, slice(128 * h, 128 * h + 128))

        loop(COUNT[g], one)

    for g in range(NG):
        loads[2 * g].wait()
        loads[2 * g + 1].wait()
        if g == 0:
            for copy in loads[2:4]:
                copy.start()
        grad_top(g)
        if g == 0:
            load_plane.wait()
            late = [load_skip, load_w1, load_xf, load_yf, load_yb, load_xb, load_lift, load_w0, load_pre0]
            for copy in loads[4:] + late:
                copy.start()
        forward_zt(g, s1[g])
        if g == 0:
            pl.semaphore_wait(barrier, NA + NB - 2)
        send("aa", s1[g], r1[g], g)

    def spread(rows, groups):
        r = lax.broadcasted_iota(jnp.int32, (rows, groups), 0) // 16
        return (r == lax.broadcasted_iota(jnp.int32, (rows, groups), 1)).astype(BF)

    load_skip.wait()
    skip_all = skip_ref[...].astype(F32)
    left = dot_nt(spread(320, C), skip_all[:, 1, :].astype(BF)).astype(BF)
    whole = dot_nt(left, spread(320, C))
    same = lax.broadcasted_iota(jnp.int32, (320, 320), 0) % 16 == lax.broadcasted_iota(jnp.int32, (320, 320), 1) % 16
    kron[...] = jnp.where(same, whole, 0.0).astype(BF)
    load_w1.wait()

    def widen(o):
        for k in range(3):
            for t in range(4):
                part = slice(128 * t, min(128 * t + 128, 432))
                wide[o, k, :, part] = wts[1, o, :, k, :, part].reshape(40, part.stop - part.start).astype(F32)

    loop(C, widen)
    load_xf.wait()

    def stage_x1(g):
        arrive("aa", r1[g], g)
        forward_x(r1[g], s2[g], g)
        send("ba", s2[g], r2[g], 4 + g)

    stage_x1(0)

    def skip_piece1(n):
        part = pl.ds(pl.multiple_of(512 * n, 512), 512)
        for pair in range(2):
            rows = slice(16 * pair, 16 * pair + 16)
            out = dot(kron[...], g1[:, rows, part].reshape(320, 512))
            skip1[:, rows, part] = out.reshape(C, 16, 512)

    loop(4, skip_piece1)
    for g in range(1, NG):
        stage_x1(g)

    load_yf.wait()
    for g in range(NG):
        arrive("ba", r2[g], 4 + g)
        forward_y(r2[g], g)
        mix(g)

    load_yb.wait()
    for g in range(NG):
        unmix(g)
        back_y(s3[g], g)
        send("ba", s3[g], r3[g], 8 + g)

    load_lift.wait()
    for i in range(C):
        lift_rows[i] = jnp.broadcast_to(lift_ref[:, i : i + 1], (2, 128))
    load_w0.wait()

    def fold_weights(k):
        for t in range(4):
            part = slice(128 * t, min(128 * t + 128, 432))
            size = part.stop - part.start
            for o in range(C):
                total = wts[0, o, 0, k, :, part].astype(F32) * lift_rows[0, :, 0:size]
                for i in range(1, C):
                    total = total + wts[0, o, i, k, :, part].astype(F32) * lift_rows[i, :, 0:size]
                weff[k, 0, o : o + 1, part] = total[0:1]
                weff[k, 1, o : o + 1, part] = total[1:2]

    loop(3, fold_weights)
    load_xb.wait()
    for g in range(NG):
        arrive("ba", r3[g], 8 + g)
        out = back_x(r3[g][...].reshape(256, WIDTH[g]))
        s4[g][...] = out.astype(BF).reshape(NA, 32, WIDTH[g])
        send("aa", s4[g], r4[g], 12 + g)

    load_pre0.wait()

    def slope_one(c):
        for pair in range(2):
            for n in range(4):
                part = slice(512 * n, 512 * n + 512)
                v = pre[0, c, 2 * pair : 2 * pair + 2, :, part].astype(F32).reshape(16, 512)
                slope0[c, 16 * pair : 16 * pair + 16, part] = slope_of(v)

    loop(C, slope_one)

    for g in range(NG):
        size = WIDTH[g]
        rows = slice(START[g], START[g] + 8)
        for m in range(18):
            for p in range(2):
                parts = []
                for k in range(3):
                    value = tile_of(lambda t: weff[k, p, rows, 128 * t : 128 * t + 128], m)
                    shift = (24 * k - 24 * m) % 128
                    parts.append(pltpu.roll(value, shift, 1) if shift else value)
                row = jnp.where(lane < 24, parts[0], jnp.where(lane < 48, parts[1], parts[2]))
                mt[pl.ds(2 * m + p, 8, stride=LM), :] = jnp.where(row8 < COUNT[g], row, 0.0)
        turned = mt[0:size].T[0:80]
        lifted[g, 0, :, 0:size] = turned
        lifted[g, 1, :, 0:size] = -swap(turned)

    for g in range(NG):
        arrive("aa", r4[g], 12 + g)
        unpack(r4[g], COUNT[g])
        for h in range(2):
            shifts = inverse_zt(COUNT[g], h)
            for c in range(COUNT[g]):
                o = START[g] + c
                fields = []
                for n in range(4):
                    part = slice(512 * n + 256 * h, 512 * n + 256 * h + 256)
                    incoming = skip1[o, :, part] + shifts[n][32 * c : 32 * c + 32] * SCALE_ZT
                    value = (incoming * slope0[o, :, part]).astype(BF)
                    g0[o, :, part] = value
                    fields.append(value.astype(F32))
                combine(fields, slice(32 * c, 32 * c + 32), slice(256 * h, 256 * h + 256))
        forward_zt(g, t1[g])
        send("aa", t1[g], q1[g], 16 + g)

    for g in range(NG):
        arrive("aa", q1[g], 16 + g)
        forward_x(q1[g], t2[g], g)
        send("ba", t2[g], q2[g], 20 + g)

    gain = jnp.sum(skip_all[:, 0, :] * lift_ref[...], 1, keepdims=True)

    def skip_piece(n):
        part = pl.ds(pl.multiple_of(512 * n, 512), 512)
        for pair in range(2):
            rows = slice(16 * pair, 16 * pair + 16)
            total = jnp.zeros((16, 512), F32)
            for c in range(C):
                total = total + g0[c, rows, part].astype(F32) * gain[c : c + 1, :]
            out_ref[rows, part] = total

    loop(4, skip_piece)

    for g in range(NG):
        arrive("ba", q2[g], 20 + g)
        part = slice(0, WIDTH[g])
        out = spectrum_y(q2[g], g)
        fold[0, :, part] += out * lifted[g, 0, :, part]
        fold[1, :, part] += out * lifted[g, 1, :, part]

    pairs = []
    for t in range(2):
        real, imag = fold[0, :, 128 * t : 128 * t + 128], fold[1, :, 128 * t : 128 * t + 128]
        real = real + pltpu.roll(real, 127, 1)
        imag = imag + pltpu.roll(imag, 1, 1)
        pairs.append(jnp.where(lanes(80) % 2 == 0, real, imag))
    total = pairs[0]
    for c in range(1, 7):
        value = pairs[0] if LM * c + LM <= 128 else pairs[1]
        if c == 3:
            value = jnp.where(lanes(80) < 64, pairs[1], pairs[0])
        total = total + pltpu.roll(value, (-LM * c) % 128, 1)
    values = jnp.concatenate([total, jnp.zeros((48, 128), F32)], 0).astype(BF)
    out = dot(yb_ref[0], values) - swap(dot(yb_ref[1], values))
    t3[...] = out.astype(BF).reshape(NB, 32, 128)
    send("ba", t3, q3, 24)
    arrive("ba", q3, 24)
    t4[...] = back_x(q3[...].reshape(256, 128)).astype(BF).reshape(NA, 32, 128)
    send("aa", t4, q4, 25)
    arrive("aa", q4, 25)
    unpack(q4, 1)
    for h in range(2):
        for n, value in enumerate(inverse_zt(1, h)):
            out_ref[:, 512 * n + 256 * h : 512 * n + 256 * h + 256] += value * SCALE_ZT

    for g in range(NG):
        drain("aa", s1[g], g)
        drain("ba", s2[g], 4 + g)
        drain("ba", s3[g], 8 + g)
        drain("aa", s4[g], 12 + g)
        drain("aa", t1[g], 16 + g)
        drain("ba", t2[g], 20 + g)
    drain("ba", t3, 24)
    drain("aa", t4, 25)


def per_device(cotangent, pre_activations, spectral_weights, skip_weights, lift_weights):
    bf = lambda table: jnp.asarray(table.astype(np.float32), dtype=BF)
    forward_x_table = x_table()
    back_x_table = forward_x_table.transpose(0, 2, 1) / 64
    any_spec = pl.BlockSpec(memory_space=pl.ANY)
    kinds = [NA, NA, NB, NB, NB, NB, NA, NA, NA, NA, NB, NB]
    scratch = [
        pltpu.VMEM((C, 4, 8, NZT), BF),
        pltpu.VMEM((2, C, 4, 8, NZT), BF),
        pltpu.VMEM((2, C, C, 3, 2, 432), BF),
        pltpu.VMEM((C, 2, C), BF),
        pltpu.VMEM((1, C), F32),
        pltpu.VMEM((6, 512, 256), BF),
        pltpu.VMEM((2, 256, 512), BF),
        pltpu.VMEM((2, 512, 256), BF),
        pltpu.VMEM((2, 80, 256), BF),
        pltpu.VMEM((2, 256, 128), BF),
        pltpu.VMEM((C, 32, NZT), BF),
        pltpu.VMEM((C, 32, NZT), BF),
        pltpu.VMEM((C, 32, NZT), F32),
        pltpu.VMEM((C, 32, NZT), F32),
        pltpu.VMEM((4, 224, 256), BF),
        pltpu.VMEM((4, 224, 512), BF),
        pltpu.VMEM((320, 320), BF),
        pltpu.VMEM((C, 3, 40, 432), F32),
        *[pltpu.VMEM((2, size, 32, 128), BF) for size in kinds],
        *[pltpu.VMEM((2, size, 32, 256), BF) for size in kinds],
        pltpu.VMEM((NB, 32, 128), BF), pltpu.VMEM((NB, 32, 128), BF),
        pltpu.VMEM((NA, 32, 128), BF), pltpu.VMEM((NA, 32, 128), BF),
        pltpu.VMEM((296, 128), F32),
        pltpu.VMEM((3, 2, NG, 8, 512), F32),
        pltpu.VMEM((3, 2, 4, 56, 128), F32),
        pltpu.VMEM((3, 2, 8, 512), F32),
        pltpu.VMEM((296, 128), F32),
        pltpu.VMEM((3, 2, 32, 512), F32),
        pltpu.VMEM((2, 80, 256), F32),
        pltpu.VMEM((NG, 2, 80, 256), F32),
        pltpu.VMEM((C, 2, 128), F32),
        pltpu.SemaphoreType.DMA((19,)),
        pltpu.SemaphoreType.DMA((26,)),
        pltpu.SemaphoreType.DMA((26,)),
    ]
    out = pl.pallas_call(
        kernel,
        out_shape=jax.ShapeDtypeStruct((32, NZT), F32),
        in_specs=[any_spec] * 10,
        out_specs=pl.BlockSpec(memory_space=pltpu.VMEM),
        scratch_shapes=scratch,
        compiler_params=pltpu.CompilerParams(
            collective_id=0, has_side_effects=True, vmem_limit_bytes=66000000
        ),
        name="fno_grad",
    )(
        cotangent.reshape(C, 4, 8, NZT),
        pre_activations.reshape(2, C, 4, 8, NZT),
        spectral_weights.transpose(0, 2, 3, 4, 1, 5),
        skip_weights.transpose(1, 0, 2),
        lift_weights.reshape(1, C),
        bf(plane_table()),
        bf(forward_x_table),
        bf(back_x_table),
        bf(y_table()),
        bf(y_back_table()),
    )
    return out.reshape(1, 4, 8, NZT)


def solution(mesh):
    return jax.shard_map(
        per_device,
        mesh=mesh,
        in_specs=(
            P(None, None, "aa", "ba", None),
            P(None, None, None, "aa", "ba", None),
            P(None, None, None, None, "ba", "aa"),
            P(),
            P(),
        ),
        out_specs=P(None, "aa", "ba", None),
        check_vma=False,
    )
```

```python
import math

import jax
import jax.numpy as jnp
import numpy as np
from jax import lax
from jax.experimental import pallas as pl
from jax.experimental.pallas import tpu as pltpu
from jax.sharding import PartitionSpec as P

C = 20
NZT = 2048
NA = 16
NB = 8
NG = 4
START = (0, 3, 10, 17)
COUNT = (3, 7, 7, 3)
WIDTH = (128, 256, 256, 128)
LM = 36
SCALE_ZT = 1.0 / NZT
BF = jnp.bfloat16
F32 = jnp.float32
INV_SQRT2 = 1.0 / math.sqrt(2.0)
INV_SQRT2PI = 1.0 / math.sqrt(2.0 * math.pi)


def freq(count):
    j = np.arange(count)
    return np.where(j < count // 2, j, j - count)


def plane_table():
    cell = np.arange(512)
    kt = np.arange(12)
    table = np.zeros((6, 512, 256))
    for f in range(24):
        kz, rest, place = freq(24)[f], f % 4, f // 4
        column = (24 * place if place < 5 else 128) + 2 * kt
        turns = (kz * (cell[:, None] // 32) * 32 + kt[None, :] * (cell[:, None] % 32) * 64) % NZT
        angle = 2.0 * np.pi / NZT * turns
        index = {0: 0, 2: 1, 1: 2, 3: 3}[rest]
        table[index][:, column] = np.cos(angle)
        table[index][:, column + 1] = -np.sin(angle)
        if rest % 2:
            sign = -1 if rest == 1 else 1
            table[index + 2][:, column] = sign * np.sin(angle)
            table[index + 2][:, column + 1] = sign * np.cos(angle)
    return table


CLASS = (0, 2, 1, 3)


def slot(f):
    return 24 * (f // 4) if f < 20 else 128


def pieces_of(a):
    u = a // 2
    if a % 2 == 0:
        return [(3 * u, 0, 24, 0), (3 * u + 1, 0, 12, 24)]
    return [(3 * u + 1, 12, 12, 0), (3 * u + 2, 0, 24, 12)]


def line_angle():
    return 2.0 * np.pi / 64 * ((freq(24)[:, None] * np.arange(64)[None, :]) % 64)


def x_table():
    angle = line_angle()
    out = np.zeros((2, NB, 4, 8, 64, 8))
    for y in range(8):
        out[0, :, :3, y, :, y] = np.cos(angle).reshape(NB, 3, 64)
        out[1, :, :3, y, :, y] = np.sin(angle).reshape(NB, 3, 64)
    return out.reshape(2, 256, 512)


def y_table():
    angle = line_angle().reshape(24, NB, 8)
    out = np.zeros((2, 80, NB, 4, 8))
    for k in range(3):
        out[0, 24 * k : 24 * k + 24, :, k] = np.cos(angle)
        out[1, 24 * k : 24 * k + 24, :, k] = np.sin(angle)
    return out.reshape(2, 80, 256)


def y_back_table():
    wide = np.zeros((2, 256, 128))
    wide[:, :, :80] = y_table().transpose(0, 2, 1) / 64
    return wide


def swap(values):
    even = lax.broadcasted_iota(jnp.int32, (values.shape[0], 128), 1) % 2 == 0
    parts = []
    for t in range(values.shape[1] // 128):
        part = values[:, 128 * t : 128 * t + 128]
        parts.append(jnp.where(even, pltpu.roll(part, 127, 1), -pltpu.roll(part, 1, 1)))
    return parts[0] if len(parts) == 1 else jnp.concatenate(parts, 1)


def dot(a, b):
    return jnp.dot(a, b, preferred_element_type=F32)


def dot_nt(a, b):
    return lax.dot_general(a, b, (((1,), (1,)), ((), ())), preferred_element_type=F32)


def slope_of(v):
    normal_cdf = 0.5 + 0.5 * lax.erf(v * INV_SQRT2)
    return normal_cdf + v * (jnp.exp(-0.5 * v * v) * INV_SQRT2PI)


def loop(count, body):
    lax.fori_loop(0, count, lambda i, carry: (body(i), carry)[1], 0)


def kernel(
    cot_h, pre_h, wts_h, skip_h, lift_h, plane_h, xf_h, xb_h, yf_h, yb_h, out_ref,
    cot, pre, wts, skip_ref, lift_ref, plane, xf, xb, yf_ref, yb_ref,
    g1, g0, slope0, skip1, bx, pz, kron, wide,
    s1n, r1n, s2n, r2n, s3n, r3n, s4n, r4n, t1n, q1n, t2n, q2n,
    s1w, r1w, s2w, r2w, s3w, r3w, s4w, r4w, t1w, q1w, t2w, q2w,
    t3, q3, t4, q4, q5,
    q, sm, mm, mg, mt, weff, fold, lifted, lift_rows,
    in_sem, send_sem, recv_sem,
):
    me_a = lax.axis_index("aa")
    me_b = lax.axis_index("ba")
    lane = lax.broadcasted_iota(jnp.int32, (8, 128), 1)
    row8 = lax.broadcasted_iota(jnp.int32, (8, 128), 0)

    def lanes(rows):
        return lax.broadcasted_iota(jnp.int32, (rows, 128), 1)

    def boxes(narrow, wide_box):
        return [narrow.at[0], wide_box.at[0], wide_box.at[1], narrow.at[1]]

    s1, r1, s2, r2 = boxes(s1n, s1w), boxes(r1n, r1w), boxes(s2n, s2w), boxes(r2n, r2w)
    s3, r3, s4, r4 = boxes(s3n, s3w), boxes(r3n, r3w), boxes(s4n, s4w), boxes(r4n, r4w)
    t1, q1, t2, q2 = boxes(t1n, t1w), boxes(q1n, q1w), boxes(t2n, t2w), boxes(q2n, q2w)

    loads = []
    for g in range(NG):
        part = pl.ds(START[g], COUNT[g])
        loads.append(pltpu.make_async_copy(cot_h.at[part], cot.at[part], in_sem.at[2 * g]))
        loads.append(pltpu.make_async_copy(pre_h.at[1, part], pre.at[1, part], in_sem.at[2 * g + 1]))
    load_plane = pltpu.make_async_copy(plane_h, plane, in_sem.at[8])
    load_pre0 = pltpu.make_async_copy(pre_h.at[0], pre.at[0], in_sem.at[9])
    load_xf = pltpu.make_async_copy(xf_h, xf, in_sem.at[10])
    load_xb = pltpu.make_async_copy(xb_h, xb, in_sem.at[11])
    load_w1 = pltpu.make_async_copy(wts_h.at[1], wts.at[1], in_sem.at[12])
    load_w0 = pltpu.make_async_copy(wts_h.at[0], wts.at[0], in_sem.at[13])
    load_yf = pltpu.make_async_copy(yf_h, yf_ref, in_sem.at[14])
    load_yb = pltpu.make_async_copy(yb_h, yb_ref, in_sem.at[15])
    load_skip = pltpu.make_async_copy(skip_h, skip_ref, in_sem.at[16])
    load_lift = pltpu.make_async_copy(lift_h, lift_ref, in_sem.at[17])
    loads[0].start()
    loads[1].start()
    load_plane.start()

    barrier = pltpu.get_barrier_semaphore()

    def greet_a(d):
        peer = lax.rem(me_a + d + 1, NA)
        pl.semaphore_signal(barrier, 1, device_id={"aa": peer}, device_id_type=pl.DeviceIdType.MESH)

    def greet_b(d):
        peer = lax.rem(me_b + d + 1, NB)
        pl.semaphore_signal(barrier, 1, device_id={"ba": peer}, device_id_type=pl.DeviceIdType.MESH)

    loop(NA - 1, greet_a)
    loop(NB - 1, greet_b)

    for box in (r2n, r3n, q2n, r2w, r3w, q2w, q3):
        box[..., 24:32, :] = jnp.zeros(box.shape[:-2] + (8, box.shape[-1]), BF)
    mm[...] = jnp.zeros(mm.shape, F32)
    mt[...] = jnp.zeros(mt.shape, F32)
    weff[...] = jnp.zeros(weff.shape, F32)
    fold[...] = jnp.zeros(fold.shape, F32)
    sm[...] = jnp.zeros(sm.shape, F32)

    def partners(axis):
        if axis == "aa":
            order = [
                (1, 2, 0), (1, 2, 1), (1, 1, 0), (1, 3, 0), (1, 1, 1), (1, 3, 1), (1, 0, 0), (1, 0, 1),
                (0, 2, 0), (0, 2, 1), (0, 1, 0), (0, 3, 0), (0, 1, 1), (0, 3, 1), (0, 0, 1),
            ]
            z, x, core = me_a // 8, lax.rem(me_a // 2, 4), lax.rem(me_a, 2)
            return [
                lax.rem(z + dz, 2) * 8 + lax.rem(x + dx, 4) * 2 + lax.rem(core + dc, 2)
                for dz, dx, dc in order
            ]
        z, y = me_b // 4, lax.rem(me_b, 4)
        order = [(1, 2), (0, 2), (1, 1), (1, 3), (0, 1), (0, 3), (1, 0)]
        return [lax.rem(z + dz, 2) * 4 + lax.rem(y + dy, 4) for dz, dy in order]

    def send(axis, src, dst, slot):
        me = me_a if axis == "aa" else me_b
        rows = pl.ds(0, src.shape[1] if axis == "aa" else 24)
        for peer in partners(axis):
            pltpu.make_async_remote_copy(
                src_ref=src.at[peer, rows],
                dst_ref=dst.at[me, rows],
                send_sem=send_sem.at[slot],
                recv_sem=recv_sem.at[slot],
                device_id={axis: peer},
                device_id_type=pl.DeviceIdType.MESH,
            ).start()
        dst[me] = src[me]

    def span(axis, box):
        if axis == "aa":
            return box.at[pl.ds(0, NA - 1)]
        return box.at[pl.ds(0, NB - 1), pl.ds(0, 24)]

    def arrive(axis, dst, slot):
        part = span(axis, dst)
        pltpu.make_async_copy(part, part, recv_sem.at[slot]).wait()

    def drain(axis, src, slot):
        part = span(axis, src)
        pltpu.make_async_copy(part, part, send_sem.at[slot]).wait()

    def combine(fields, rows, part):
        sum02, sum13 = fields[0] + fields[2], fields[1] + fields[3]
        pz[0, rows, part] = (sum02 + sum13).astype(BF)
        pz[1, rows, part] = (sum02 - sum13).astype(BF)
        pz[2, rows, part] = (fields[0] - fields[2]).astype(BF)
        pz[3, rows, part] = (fields[1] - fields[3]).astype(BF)

    def forward_zt(g, dst):
        rows = slice(0, 32 * COUNT[g])
        odd, turned = pz[2, rows], pz[3, rows]
        out = [
            dot(pz[0, rows], plane[0]),
            dot(pz[1, rows], plane[1]),
            dot(odd, plane[2]) + dot(turned, plane[4]),
            dot(odd, plane[3]) + dot(turned, plane[5]),
        ]
        for a in range(NA):
            low = high = None
            for c in range(COUNT[g]):
                for f, first, size, place in pieces_of(a):
                    t, source = divmod(slot(f) + first, 128)
                    start = LM * c + place
                    piece = out[CLASS.index(f % 4)][32 * c : 32 * c + 32, 128 * t : 128 * t + 128]
                    shift = (start - source) % 128
                    if shift:
                        piece = pltpu.roll(piece, shift, 1)
                    if start < 128:
                        low = piece if low is None else jnp.where(lanes(32) < start, low, piece)
                    if start + size > 128:
                        high = piece if high is None else jnp.where(lanes(32) < start - 128, high, piece)
            dst[a, :, 0:128] = low.astype(BF)
            if high is not None:
                dst[a, :, 128:256] = high.astype(BF)

    def forward_x(src, dst, g):
        values = src[...].reshape(512, WIDTH[g])
        out = dot(xf[0], values) + swap(dot(xf[1], values))
        dst[...] = out.astype(BF).reshape(NB, 32, WIDTH[g])

    def spectrum_y(src, g):
        values = src[...].reshape(256, WIDTH[g])
        return dot(yf_ref[0], values) + swap(dot(yf_ref[1], values))

    def forward_y(src, g):
        size = WIDTH[g]
        out = spectrum_y(src, g)
        full = jnp.concatenate([out, jnp.zeros((48, size), F32)], 0)
        q[0:size] = full.T
        for p in range(2):
            tiles = [[None] * 4 for _ in range(3)]
            for m in range(18):
                rows = q[pl.ds(2 * m + p, 8, stride=LM), :]
                t, off = divmod(24 * m, 128)
                for k in range(3):
                    shift = (24 * m - 24 * k) % 128
                    piece = pltpu.roll(rows, shift, 1) if shift else rows
                    old = tiles[k][t]
                    tiles[k][t] = piece if old is None else jnp.where(lane < off, old, piece)
                    if off + 24 > 128:
                        tiles[k][t + 1] = piece
            for k in range(3):
                for t in range(4):
                    sm[k, p, g, :, 128 * t : 128 * t + 128] = tiles[k][t]

    def mix(g):
        def one(k):
            for t in range(4):
                size = 128 if t < 3 else 48
                part = slice(128 * t, 128 * t + size)
                by_re = mm[k, 0, t, 0:40, 0:size]
                by_im = mm[k, 1, t, 0:40, 0:size]
                all_re = sm[k, 0, g, :, part]
                all_im = sm[k, 1, g, :, part]
                for c in range(COUNT[g]):
                    w = wide[START[g] + c, k, :, part]
                    by_re = by_re + w * all_re[c : c + 1]
                    by_im = by_im + w * all_im[c : c + 1]
                mm[k, 0, t, 0:40, 0:size] = by_re
                mm[k, 1, t, 0:40, 0:size] = by_im

        loop(3, one)

    def unmix(g):
        first, second = pl.ds(2 * START[g], 8, stride=2), pl.ds(2 * START[g] + 1, 8, stride=2)
        for k in range(3):
            for t in range(4):
                part = slice(128 * t, 128 * t + 128)
                mg[k, 0, :, part] = mm[k, 0, t, first, :] + mm[k, 1, t, second, :]
                mg[k, 1, :, part] = mm[k, 1, t, first, :] - mm[k, 0, t, second, :]

    def tile_of(load, m):
        t, off = divmod(24 * m, 128)
        value = load(t)
        if off + 24 > 128:
            value = jnp.where(lane < 64, load(t + 1), value)
        return value

    def back_y(dst, g):
        for m in range(18):
            for p in range(2):
                parts = []
                for k in range(3):
                    value = tile_of(lambda t: mg[k, p, :, 128 * t : 128 * t + 128], m)
                    shift = (24 * k - 24 * m) % 128
                    parts.append(pltpu.roll(value, shift, 1) if shift else value)
                row = jnp.where(lane < 24, parts[0], jnp.where(lane < 48, parts[1], parts[2]))
                mt[pl.ds(2 * m + p, 8, stride=LM), :] = row
        values = mt[0 : WIDTH[g]].astype(BF)
        out = dot_nt(yb_ref[0], values) - swap(dot_nt(yb_ref[1], values))
        dst[...] = out.astype(BF).reshape(NB, 32, WIDTH[g])

    def back_x(values):
        turned = -swap(values.astype(F32))
        return dot(xb[0], values) + dot(xb[1], turned.astype(BF))

    def unpack(src, count):
        for c in range(count):
            for r in range(4):
                for t in range(2):
                    full = None
                    for f in [r, 4 + r, 8 + r, 12 + r, 16 + r] if t == 0 else [20 + r]:
                        for a in (f // 3 * 2, f // 3 * 2 + 1):
                            for kz, first, size, place in pieces_of(a):
                                if kz != f:
                                    continue
                                low, source = divmod(LM * c + place, 128)
                                value = src[a, :, 128 * low : 128 * low + 128].astype(F32)
                                if source + size > 128:
                                    value = jnp.where(lanes(32) < 64, src[a, :, 128:256].astype(F32), value)
                                start = (slot(f) + first) % 128
                                shift = (start - source) % 128
                                value = pltpu.roll(value, shift, 1) if shift else value
                                full = value if full is None else jnp.where(lanes(32) < start, full, value)
                    bx[CLASS.index(r), 32 * c : 32 * c + 32, 128 * t : 128 * t + 128] = full.astype(BF)

    def inverse_zt(count, h):
        rows, part = slice(0, 32 * count), slice(256 * h, 256 * h + 256)
        even = dot_nt(bx[0, rows], plane[0, part])
        half = dot_nt(bx[1, rows], plane[1, part])
        odd = dot_nt(bx[2, rows], plane[2, part]) + dot_nt(bx[3, rows], plane[3, part])
        turn = dot_nt(bx[2, rows], plane[4, part]) + dot_nt(bx[3, rows], plane[5, part])
        total, rest = even + half, even - half
        return [total + odd, rest + turn, total - odd, rest - turn]

    def grad_top(g):
        def one(i):
            c = START[g] + i
            for pair in range(2):
                for h in range(4):
                    fields = []
                    for n in range(4):
                        part = slice(512 * n + 128 * h, 512 * n + 128 * h + 128)
                        v = pre[1, c, 2 * pair : 2 * pair + 2, :, part].astype(F32).reshape(16, 128)
                        d = cot[c, 2 * pair : 2 * pair + 2, :, part].astype(F32).reshape(16, 128)
                        value = (d * slope_of(v)).astype(BF)
                        g1[c, 16 * pair : 16 * pair + 16, part] = value
                        fields.append(value.astype(F32))
                    rows = pl.ds(pl.multiple_of(32 * i + 16 * pair, 16), 16)
                    combine(fields, rows, slice(128 * h, 128 * h + 128))

        loop(COUNT[g], one)

    for g in range(NG):
        loads[2 * g].wait()
        loads[2 * g + 1].wait()
        if g == 0:
            for copy in loads[2:4]:
                copy.start()
        grad_top(g)
        if g == 0:
            load_plane.wait()
            late = [load_skip, load_w1, load_xf, load_yf, load_yb, load_xb, load_lift, load_w0, load_pre0]
            for copy in loads[4:] + late:
                copy.start()
        forward_zt(g, s1[g])
        if g == 0:
            pl.semaphore_wait(barrier, NA + NB - 2)
        send("aa", s1[g], r1[g], g)

    def spread(rows, groups):
        r = lax.broadcasted_iota(jnp.int32, (rows, groups), 0) // 16
        return (r == lax.broadcasted_iota(jnp.int32, (rows, groups), 1)).astype(BF)

    load_skip.wait()
    skip_all = skip_ref[...].astype(F32)
    left = dot_nt(spread(320, C), skip_all[:, 1, :].astype(BF)).astype(BF)
    whole = dot_nt(left, spread(320, C))
    same = lax.broadcasted_iota(jnp.int32, (320, 320), 0) % 16 == lax.broadcasted_iota(jnp.int32, (320, 320), 1) % 16
    kron[...] = jnp.where(same, whole, 0.0).astype(BF)
    load_w1.wait()

    def widen(o):
        for k in range(3):
            for t in range(4):
                part = slice(128 * t, min(128 * t + 128, 432))
                wide[o, k, :, part] = wts[1, o, :, k, :, part].reshape(40, part.stop - part.start).astype(F32)

    loop(C, widen)
    load_xf.wait()

    def stage_x1(g):
        arrive("aa", r1[g], g)
        forward_x(r1[g], s2[g], g)
        send("ba", s2[g], r2[g], 4 + g)

    stage_x1(0)

    def skip_piece1(n):
        part = pl.ds(pl.multiple_of(512 * n, 512), 512)
        for pair in range(2):
            rows = slice(16 * pair, 16 * pair + 16)
            out = dot(kron[...], g1[:, rows, part].reshape(320, 512))
            skip1[:, rows, part] = out.reshape(C, 16, 512)

    loop(4, skip_piece1)
    for g in range(1, NG):
        stage_x1(g)

    load_yf.wait()
    for g in range(NG):
        arrive("ba", r2[g], 4 + g)
        forward_y(r2[g], g)
        mix(g)

    load_yb.wait()
    for g in range(NG):
        unmix(g)
        back_y(s3[g], g)
        send("ba", s3[g], r3[g], 8 + g)

    load_lift.wait()
    for i in range(C):
        lift_rows[i] = jnp.broadcast_to(lift_ref[:, i : i + 1], (2, 128))
    load_w0.wait()

    def fold_weights(k):
        for t in range(4):
            part = slice(128 * t, min(128 * t + 128, 432))
            size = part.stop - part.start
            for o in range(C):
                total = wts[0, o, 0, k, :, part].astype(F32) * lift_rows[0, :, 0:size]
                for i in range(1, C):
                    total = total + wts[0, o, i, k, :, part].astype(F32) * lift_rows[i, :, 0:size]
                weff[k, 0, o : o + 1, part] = total[0:1]
                weff[k, 1, o : o + 1, part] = total[1:2]

    loop(3, fold_weights)
    load_xb.wait()
    for g in range(NG):
        arrive("ba", r3[g], 8 + g)
        out = back_x(r3[g][...].reshape(256, WIDTH[g]))
        s4[g][...] = out.astype(BF).reshape(NA, 32, WIDTH[g])
        send("aa", s4[g], r4[g], 12 + g)

    load_pre0.wait()

    def slope_one(c):
        for pair in range(2):
            for n in range(4):
                part = slice(512 * n, 512 * n + 512)
                v = pre[0, c, 2 * pair : 2 * pair + 2, :, part].astype(F32).reshape(16, 512)
                slope0[c, 16 * pair : 16 * pair + 16, part] = slope_of(v)

    loop(C, slope_one)

    for g in range(NG):
        size = WIDTH[g]
        rows = slice(START[g], START[g] + 8)
        for m in range(18):
            for p in range(2):
                parts = []
                for k in range(3):
                    value = tile_of(lambda t: weff[k, p, rows, 128 * t : 128 * t + 128], m)
                    shift = (24 * k - 24 * m) % 128
                    parts.append(pltpu.roll(value, shift, 1) if shift else value)
                row = jnp.where(lane < 24, parts[0], jnp.where(lane < 48, parts[1], parts[2]))
                mt[pl.ds(2 * m + p, 8, stride=LM), :] = jnp.where(row8 < COUNT[g], row, 0.0)
        turned = mt[0:size].T[0:80]
        lifted[g, 0, :, 0:size] = turned
        lifted[g, 1, :, 0:size] = -swap(turned)

    for g in range(NG):
        arrive("aa", r4[g], 12 + g)
        unpack(r4[g], COUNT[g])
        for h in range(2):
            shifts = inverse_zt(COUNT[g], h)
            for c in range(COUNT[g]):
                o = START[g] + c
                fields = []
                for n in range(4):
                    part = slice(512 * n + 256 * h, 512 * n + 256 * h + 256)
                    incoming = skip1[o, :, part] + shifts[n][32 * c : 32 * c + 32] * SCALE_ZT
                    value = (incoming * slope0[o, :, part]).astype(BF)
                    g0[o, :, part] = value
                    fields.append(value.astype(F32))
                combine(fields, slice(32 * c, 32 * c + 32), slice(256 * h, 256 * h + 256))
        forward_zt(g, t1[g])
        send("aa", t1[g], q1[g], 16 + g)

    for g in range(NG):
        arrive("aa", q1[g], 16 + g)
        forward_x(q1[g], t2[g], g)
        send("ba", t2[g], q2[g], 20 + g)

    gain = jnp.sum(skip_all[:, 0, :] * lift_ref[...], 1, keepdims=True)

    def skip_piece(n):
        part = pl.ds(pl.multiple_of(512 * n, 512), 512)
        for pair in range(2):
            rows = slice(16 * pair, 16 * pair + 16)
            total = jnp.zeros((16, 512), F32)
            for c in range(C):
                total = total + g0[c, rows, part].astype(F32) * gain[c : c + 1, :]
            out_ref[rows, part] = total

    loop(4, skip_piece)

    for g in range(NG):
        arrive("ba", q2[g], 20 + g)
        part = slice(0, WIDTH[g])
        out = spectrum_y(q2[g], g)
        fold[0, :, part] += out * lifted[g, 0, :, part]
        fold[1, :, part] += out * lifted[g, 1, :, part]

    pairs = []
    for t in range(2):
        real, imag = fold[0, :, 128 * t : 128 * t + 128], fold[1, :, 128 * t : 128 * t + 128]
        real = real + pltpu.roll(real, 127, 1)
        imag = imag + pltpu.roll(imag, 1, 1)
        pairs.append(jnp.where(lanes(80) % 2 == 0, real, imag))
    total = pairs[0]
    for c in range(1, 7):
        value = pairs[0] if LM * c + LM <= 128 else pairs[1]
        if c == 3:
            value = jnp.where(lanes(80) < 64, pairs[1], pairs[0])
        total = total + pltpu.roll(value, (-LM * c) % 128, 1)
    values = jnp.concatenate([total, jnp.zeros((48, 128), F32)], 0).astype(BF)
    out = dot(yb_ref[0], values) - swap(dot(yb_ref[1], values))
    t3[...] = out.astype(BF).reshape(NB, 32, 128)
    send("ba", t3, q3, 24)
    arrive("ba", q3, 24)
    full = back_x(q3[...].reshape(256, 128)).reshape(NA, 4, 8, 128)
    x0, x1, x2, x3 = [full[:, i].reshape(128, 128) for i in range(4)]
    wide_lane = lanes(128)
    x2 = pltpu.roll(x2, 2 * LM, 1)
    x0 = jnp.where(wide_lane < LM, x0, jnp.where(wide_lane < 2 * LM, pltpu.roll(x1, LM, 1), x2))
    t4[:, 0:8] = x0.astype(BF).reshape(NA, 8, 128)
    t4[:, 8:16] = x3.astype(BF).reshape(NA, 8, 128)
    send("aa", t4, q4, 25)
    arrive("aa", q4, 25)
    shared = q4[:, 0:8].astype(F32).reshape(128, 128)
    q5[:, 0:8] = shared.reshape(NA, 8, 128)
    q5[:, 8:16] = pltpu.roll(shared, 128 - LM, 1).reshape(NA, 8, 128)
    q5[:, 16:24] = pltpu.roll(shared, 128 - 2 * LM, 1).reshape(NA, 8, 128)
    q5[:, 24:32] = q4[:, 8:16].astype(F32)
    unpack(q5, 1)
    for h in range(2):
        for n, value in enumerate(inverse_zt(1, h)):
            out_ref[:, 512 * n + 256 * h : 512 * n + 256 * h + 256] += value * SCALE_ZT

    for g in range(NG):
        drain("aa", s1[g], g)
        drain("ba", s2[g], 4 + g)
        drain("ba", s3[g], 8 + g)
        drain("aa", s4[g], 12 + g)
        drain("aa", t1[g], 16 + g)
        drain("ba", t2[g], 20 + g)
    drain("ba", t3, 24)
    drain("aa", t4, 25)


def per_device(cotangent, pre_activations, spectral_weights, skip_weights, lift_weights):
    bf = lambda table: jnp.asarray(table.astype(np.float32), dtype=BF)
    forward_x_table = x_table()
    back_x_table = forward_x_table.transpose(0, 2, 1) / 64
    any_spec = pl.BlockSpec(memory_space=pl.ANY)
    kinds = [NA, NA, NB, NB, NB, NB, NA, NA, NA, NA, NB, NB]
    scratch = [
        pltpu.VMEM((C, 4, 8, NZT), BF),
        pltpu.VMEM((2, C, 4, 8, NZT), BF),
        pltpu.VMEM((2, C, C, 3, 2, 432), BF),
        pltpu.VMEM((C, 2, C), BF),
        pltpu.VMEM((1, C), F32),
        pltpu.VMEM((6, 512, 256), BF),
        pltpu.VMEM((2, 256, 512), BF),
        pltpu.VMEM((2, 512, 256), BF),
        pltpu.VMEM((2, 80, 256), BF),
        pltpu.VMEM((2, 256, 128), BF),
        pltpu.VMEM((C, 32, NZT), BF),
        pltpu.VMEM((C, 32, NZT), BF),
        pltpu.VMEM((C, 32, NZT), F32),
        pltpu.VMEM((C, 32, NZT), F32),
        pltpu.VMEM((4, 224, 256), BF),
        pltpu.VMEM((4, 224, 512), BF),
        pltpu.VMEM((320, 320), BF),
        pltpu.VMEM((C, 3, 40, 432), F32),
        *[pltpu.VMEM((2, size, 32, 128), BF) for size in kinds],
        *[pltpu.VMEM((2, size, 32, 256), BF) for size in kinds],
        pltpu.VMEM((NB, 32, 128), BF), pltpu.VMEM((NB, 32, 128), BF),
        pltpu.VMEM((NA, 16, 128), BF), pltpu.VMEM((NA, 16, 128), BF),
        pltpu.VMEM((NA, 32, 128), F32),
        pltpu.VMEM((296, 128), F32),
        pltpu.VMEM((3, 2, NG, 8, 512), F32),
        pltpu.VMEM((3, 2, 4, 56, 128), F32),
        pltpu.VMEM((3, 2, 8, 512), F32),
        pltpu.VMEM((296, 128), F32),
        pltpu.VMEM((3, 2, 32, 512), F32),
        pltpu.VMEM((2, 80, 256), F32),
        pltpu.VMEM((NG, 2, 80, 256), F32),
        pltpu.VMEM((C, 2, 128), F32),
        pltpu.SemaphoreType.DMA((19,)),
        pltpu.SemaphoreType.DMA((26,)),
        pltpu.SemaphoreType.DMA((26,)),
    ]
    out = pl.pallas_call(
        kernel,
        out_shape=jax.ShapeDtypeStruct((32, NZT), F32),
        in_specs=[any_spec] * 10,
        out_specs=pl.BlockSpec(memory_space=pltpu.VMEM),
        scratch_shapes=scratch,
        compiler_params=pltpu.CompilerParams(
            collective_id=0, has_side_effects=True, vmem_limit_bytes=66000000
        ),
        name="fno_grad",
    )(
        cotangent.reshape(C, 4, 8, NZT),
        pre_activations.reshape(2, C, 4, 8, NZT),
        spectral_weights.transpose(0, 2, 3, 4, 1, 5),
        skip_weights.transpose(1, 0, 2),
        lift_weights.reshape(1, C),
        bf(plane_table()),
        bf(forward_x_table),
        bf(back_x_table),
        bf(y_table()),
        bf(y_back_table()),
    )
    return out.reshape(1, 4, 8, NZT)


def solution(mesh):
    return jax.shard_map(
        per_device,
        mesh=mesh,
        in_specs=(
            P(None, None, "aa", "ba", None),
            P(None, None, None, "aa", "ba", None),
            P(None, None, None, None, "ba", "aa"),
            P(),
            P(),
        ),
        out_specs=P(None, "aa", "ba", None),
        check_vma=False,
    )
```
